32 devices in a mesh: dp: 2 (over x), sp: 16 (over y, z, core).
Axes of the slice: x: 2, y: 2, z: 4, core: 2. Of those that a mesh axis runs over, the one named last changes fastest.
Arguments:
- x: bfloat16 [16384, 2048], P(('dp', 'sp')), parts along dimension 0
- gain: bfloat16 [2048], replicated
- wq: bfloat16 [2048, 2048], P('sp')
- wk: bfloat16 [2048, 256], P('sp')
- wv: bfloat16 [2048, 256], P('sp')
- wo: bfloat16 [2048, 2048], P('sp')
Outputs:
- output: bfloat16 [16384, 2048], P(('dp', 'sp')), parts along dimension 0
There are 2 independent parts. The reference program is written for one: setup_inputs(seed, part) draws one part's arguments, and reference() takes and returns one part's arrays. A program takes and returns all parts, laid end to end along the dimension named above; an argument that names none is the same for every part.
All inputs are finite; a program needn't handle non-finite values.
Results may differ from the reference program's by a relative error of at most 0.012.
Values are sent between devices in bfloat16 or wider.
A program may use at most 2 GiB of HBM per device.

```python
import jax
import jax.numpy as jnp
from jax import lax

ROWS = 8192
D = 2048
HEADS = 8
KV_HEADS = 1
HEAD = 256
THETA = 10000


def setup_inputs(seed: int = 0, part: int = 0) -> dict:
    kx, kn, kq, kk, kv, ko = jax.random.split(jax.random.key(seed), 6)

    def weights(key, rows, columns):
        return jax.random.normal(key, (rows, columns), jnp.float32) * rows**-0.5

    drawn = {
        "x": jax.random.normal(jax.random.fold_in(kx, part), (ROWS, D), jnp.float32),
        "gain": 1 + 0.1 * jax.random.normal(kn, (D,), jnp.float32),
        "wq": 2 * weights(kq, D, HEADS * HEAD),
        "wk": 2 * weights(kk, D, KV_HEADS * HEAD),
        "wv": 4 * weights(kv, D, KV_HEADS * HEAD),
        "wo": weights(ko, HEADS * HEAD, D),
    }
    return {k: v.astype(jnp.bfloat16) for k, v in drawn.items()}


def normed(x, gain):
    wide = x.astype(jnp.float32)
    scale = lax.rsqrt(jnp.mean(wide * wide, -1, keepdims=True) + 1e-6)
    return (wide * scale * gain.astype(jnp.float32)).astype(jnp.bfloat16)


def turned(t, place, theta):
    half = t.shape[-1] // 2
    angle = place.astype(jnp.float32)[:, None] * theta ** (-jnp.arange(half, dtype=jnp.float32) / half)
    cos, sin = jnp.cos(angle)[:, None], jnp.sin(angle)[:, None]
    a, b = t[..., :half].astype(jnp.float32), t[..., half:].astype(jnp.float32)
    return jnp.concatenate([a * cos - b * sin, b * cos + a * sin], -1).astype(jnp.bfloat16)


def matmul(a, w):
    return jnp.dot(a, w, preferred_element_type=jnp.float32).astype(jnp.bfloat16)


def einsum(form, a, b):
    return jnp.einsum(form, a.astype(jnp.float32), b.astype(jnp.float32))


def attention(q, k, v):
    scores = einsum("tgsd,ugd->gstu", q, k) * q.shape[-1] ** -0.5
    token = jnp.arange(q.shape[0])
    scores = jnp.where(token[:, None] >= token, scores, -jnp.inf)
    weights = jax.nn.softmax(scores, -1).astype(jnp.bfloat16)
    return einsum("gstu,ugd->tgsd", weights, v).astype(jnp.bfloat16)


def reference(x, gain, wq, wk, wv, wo):
    a, place = normed(x, gain), jnp.arange(ROWS)
    q = turned(matmul(a, wq).reshape(ROWS, HEADS, HEAD), place, THETA).reshape(ROWS, KV_HEADS, -1, HEAD)
    k = turned(matmul(a, wk).reshape(ROWS, KV_HEADS, HEAD), place, THETA)
    v = matmul(a, wv).reshape(ROWS, KV_HEADS, HEAD)
    seen = attention(q, k, v).reshape(ROWS, HEADS * HEAD)
    return (x.astype(jnp.float32) + jnp.dot(seen, wo, preferred_element_type=jnp.float32)).astype(jnp.bfloat16)
```

```python
import functools

import jax
import jax.numpy as jnp
from jax import lax
from jax.experimental import pallas as pl
from jax.experimental.pallas import tpu as pltpu
from jax.sharding import PartitionSpec as P

HEAD = 256
THETA = 10000
NEG = -1e30
HIDDEN = 2 * NEG
LOG2E = 1.4426950408889634
MESH = pl.DeviceIdType.MESH
CW, CCW = 0, 1
W1, KV, WO = 0, 1, 2
STEPS = (4, 3)


def _dot(a, b, ca, cb):
    return lax.dot_general(a, b, (((ca,), (cb,)), ((), ())), preferred_element_type=jnp.float32)


def _chip(p):
    y = p // 4
    return 4 * y + p + y * (7 - 2 * p)


def _lane(x, unit=128):
    return x if isinstance(x, int) else pl.multiple_of(x, unit)


def _kernel(x_hbm, gain_ref, wq_hbm, wk_hbm, wv_hbm, wo_hbm, cos_ref, sin_ref, out_ref,
            x_s, a_s, w1_s, wo_s, kv_s, acc_s, q_s, top_s, mix_s,
            local, ring_send, ring_recv, x_send, x_recv, d_send, d_recv, dx_send, dx_recv, *, shift):
    tokens, dim = x_s.shape
    depth = wq_hbm.shape[0]
    head = kv_s.shape[1] // 2
    heads = dim // head
    unit = 2 * head
    half = dim // 2
    group, me = lax.axis_index("dp"), lax.axis_index("sp")
    chip, core = me // 2, me % 2
    row = chip // 4
    z = chip % 4
    place = row * 7 + z - 2 * row * z

    def device(p):
        return (group, _chip(p % 8) * 2 + core)

    right, left, twin, mate = device(place + 1), device(place + 7), (1 - group, me), (group, chip * 2 + 1 - core)

    def origin(way, t):
        return _chip((place + 8 - t) % 8 if way == CW else (place + t) % 8)

    bufs = {W1: (w1_s, depth), KV: (kv_s, tokens), WO: (wo_s, depth)}

    def window(kind, way, t, of_core, cols):
        buf, rows = bufs[kind]
        begin, width = cols
        at = (origin(way, t) * 2 + of_core) * rows
        return buf.at[pl.ds(pl.multiple_of(at, rows), rows), pl.ds(_lane(begin), width)]

    def whole(kind):
        return (0, bufs[kind][0].shape[1])

    def ring_cols(kind):
        full = whole(kind)[1]
        return (0, full) if kind == KV else (group * shift, full - shift)

    def x_cols(kind, of_group):
        return (of_group * (whole(kind)[1] - shift), shift)

    def copy(src, send, recv, to):
        return pltpu.make_async_remote_copy(src_ref=src, dst_ref=src, send_sem=send, recv_sem=recv, device_id=to, device_id_type=MESH)

    def ring(kind, way, t, sent):
        at = t - 1 if sent else t
        return copy(window(kind, way, at, core, ring_cols(kind)), ring_send.at[kind, way, t], ring_recv.at[kind, way, t],
                    right if way == CW else left)

    def over_x(kind, way, t, sent):
        return copy(window(kind, way, t, core, x_cols(kind, group if sent else 1 - group)), x_send.at[kind, way, t], x_recv.at[kind, way, t], twin)

    def to_mate(kind, way, t, sent):
        cols = whole(kind) if isinstance(t, int) and t == 0 else ring_cols(kind)
        return copy(window(kind, way, t, core if sent else 1 - core, cols), d_send.at[kind, way, t], d_recv.at[kind, way, t], mate)

    def x_to_mate(kind, way, t, sent):
        return copy(window(kind, way, t, core if sent else 1 - core, x_cols(kind, 1 - group)), dx_send.at[kind, way, t], dx_recv.at[kind, way, t], mate)

    def begin(kind):
        ring(kind, CW, 1, True).start()
        ring(kind, CCW, 1, True).start()
        to_mate(kind, CW, 0, True).start()

    def arrive(kind, way, t):
        ring(kind, way, t, False).wait_recv()
        if isinstance(t, int):
            if t < STEPS[way]:
                ring(kind, way, t + 1, True).start()
        else:
            @pl.when(t < STEPS[way])
            def _():
                ring(kind, way, t + 1, True).start()
        if kind != KV:
            over_x(kind, way, t, True).start()
        to_mate(kind, way, t, True).start()

    def arrive_x(kind, way, t):
        over_x(kind, way, t, False).wait_recv()
        x_to_mate(kind, way, t, True).start()

    def from_mate(kind, way, t):
        to_mate(kind, way, t, False).wait_recv()

    def x_from_mate(kind, way, t):
        x_to_mate(kind, way, t, False).wait_recv()

    own = pl.ds(pl.multiple_of(me * depth, depth), depth)
    loads = [
        (wq_hbm.at[:, pl.ds(0, half)], w1_s.at[own, pl.ds(0, half)]),
        (wk_hbm, w1_s.at[own, pl.ds(half, head)]),
        (wv_hbm, w1_s.at[own, pl.ds(half + head, head)]),
        (wq_hbm.at[:, pl.ds(half, half)], w1_s.at[own, pl.ds(half + unit, half)]),
        (x_hbm, x_s),
        (wo_hbm, wo_s.at[own, :]),
    ]
    loads = [pltpu.make_async_copy(src, dst, local.at[i]) for i, (src, dst) in enumerate(loads)]
    for load in loads:
        load.start()
    barrier = pltpu.get_barrier_semaphore()
    for to in (right, left, twin, mate):
        pl.semaphore_signal(barrier, inc=1, device_id=to, device_id_type=MESH)
    for load in loads[:4]:
        load.wait()
    pl.semaphore_wait(barrier, 4)
    begin(W1)

    loads[4].wait()
    gain = gain_ref[...].astype(jnp.float32)
    some = min(64, tokens)

    def norm(i, _):
        here = pl.ds(pl.multiple_of(i * some, some), some)
        wide = x_s[here, :].astype(jnp.float32)
        scale = lax.rsqrt(jnp.mean(wide * wide, -1, keepdims=True) + 1e-6)
        a_s[here, :] = (wide * scale * gain).astype(jnp.bfloat16)

    lax.fori_loop(0, tokens // some, norm, None)

    def project(chip_of, first, count, fresh=False):
        rows = pl.ds(pl.multiple_of(chip_of * 2 * depth, 2 * depth), 2 * depth)
        cols_a = pl.ds(pl.multiple_of(chip_of * 2 * depth, 2 * depth), 2 * depth)

        def tile(n, _):
            cols = pl.ds(pl.multiple_of((first + n) * unit, unit), unit)
            term = _dot(a_s[:, cols_a], w1_s[rows, cols], 1, 0)
            acc_s[:, cols] = term if fresh else acc_s[:, cols] + term

        lax.fori_loop(0, count, tile, None)

    mid = half // unit

    def queries(way, t):
        project(origin(way, t), 0, mid)
        project(origin(way, t), mid + 1, mid)

    from_mate(W1, CW, 0)
    project(chip, 0, 2 * mid + 1, fresh=True)
    for t in (1, 2, 3, 4):
        ways = (CW, CCW) if t < 4 else (CW,)
        for way in ways:
            arrive(W1, way, t)
        if t > 1:
            for way in (CW, CCW):
                arrive_x(W1, way, t - 1)
        for way in ways:
            from_mate(W1, way, t)
            project(origin(way, t), mid, 1)
        if t > 1:
            for way in (CW, CCW):
                x_from_mate(W1, way, t - 1)
                queries(way, t - 1)

    cos, sin = cos_ref[...], sin_ref[...]

    def turned(t):
        t = t.astype(jnp.bfloat16).astype(jnp.float32)
        a, b = t[:, : head // 2], t[:, head // 2 :]
        return jnp.concatenate([a * cos - b * sin, b * cos + a * sin], -1).astype(jnp.bfloat16)

    here = pl.multiple_of(me * tokens, tokens)
    kv_s[pl.ds(here, tokens), :head] = turned(acc_s[:, half : half + head])
    part = tokens // 2
    for j in range(2):
        value = acc_s[j * part : (j + 1) * part, half + head : half + unit].astype(jnp.bfloat16)
        kv_s[pl.ds(here + j * part, part), head:] = value.T if value.shape[0] == value.shape[1] else value
    begin(KV)

    arrive_x(W1, CW, 4)
    x_from_mate(W1, CW, 4)
    queries(CW, 4)

    def turn(h, _):
        cols = pl.ds(pl.multiple_of(h * head + (h // (heads // 2)) * unit, head), head)
        q_s[pl.ds(pl.multiple_of(h * tokens, tokens), tokens), :] = turned(acc_s[:, cols])

    lax.fori_loop(0, heads, turn, None)

    e = head**-0.5 * LOG2E
    top_s[...] = jnp.full(top_s.shape, NEG, jnp.float32)
    mix_s[...] = jnp.zeros(mix_s.shape, jnp.float32)

    def block(of, masked):
        base = pl.multiple_of(of * tokens, tokens)
        keys = kv_s[pl.ds(base, tokens), :head]
        scores = [_dot(keys, q_s[h * tokens : (h + 1) * tokens, :], 1, 1) for h in range(heads)]
        ok = None
        if masked:
            ok = lax.broadcasted_iota(jnp.int32, (tokens, tokens), 0) <= lax.broadcasted_iota(jnp.int32, (tokens, tokens), 1)
        weights, keeps = [], []
        for h, s in enumerate(scores):
            at = slice(h * tokens, (h + 1) * tokens)
            if masked:
                s = jnp.where(ok, s, HIDDEN)
            old = top_s[:, at]
            top = jnp.maximum(old, s.max(axis=0, keepdims=True))
            top_s[:, at] = top
            weights.append(jnp.exp2((s - top) * e).astype(jnp.bfloat16))
            keeps.append(jnp.exp2((old - top) * e))
        values = jnp.concatenate([kv_s[pl.ds(base + j * part, part), head:] for j in range(2)], axis=1)
        values = jnp.concatenate([values, jnp.ones((8, tokens), jnp.bfloat16)], axis=0)
        for h, (p, keep) in enumerate(zip(weights, keeps)):
            at = slice(h * tokens, (h + 1) * tokens)
            mix_s[:, at] = mix_s[:, at] * keep + _dot(values, p, 1, 0)

    block(me, True)
    from_mate(KV, CW, 0)

    def step(t, _):
        @pl.when(t > 0)
        def _():
            arrive(KV, CW, t)

        @pl.when((t > 0) & (t < 4))
        def _():
            arrive(KV, CCW, t)

        @pl.when(t == 3)
        def _():
            loads[5].wait()
            begin(WO)

        def one(j, _):
            way, other = j // 2, j % 2
            there = (place + (8 - t) * (1 - way) + t * way) % 8

            @pl.when((t > 0) & (other == 1) & (way == 0))
            def _():
                to_mate(KV, CW, t, False).wait_recv()

            @pl.when((t > 0) & (t < 4) & (other == 1) & (way == 1))
            def _():
                to_mate(KV, CCW, t, False).wait_recv()

            of = _chip(there) * 2 + (1 - other) * core + other * (1 - core)

            @pl.when((of < me) & ((way == 0) | ((t > 0) & (t < 4))))
            def _():
                block(of, False)

        lax.fori_loop(0, 4, one, None)

    lax.fori_loop(0, 5, step, None)

    def finish(h, _):
        at = pl.ds(pl.multiple_of(h * tokens, tokens), tokens)
        total = mix_s[head : head + 1, at]
        a_s[:, pl.ds(pl.multiple_of(h * head, head), head)] = (mix_s[:head, at] * (1 / total)).T.astype(jnp.bfloat16)

    lax.fori_loop(0, heads, finish, None)

    def output(way, t, fresh=False):
        chip_of = origin(way, t)
        rows = pl.ds(pl.multiple_of(chip_of * 2 * depth, 2 * depth), 2 * depth)

        def tile(n, _):
            cols = pl.ds(pl.multiple_of(n * unit, unit), unit)
            term = _dot(a_s[:, rows], wo_s[rows, cols], 1, 0)
            acc_s[:, cols] = (x_s[:, cols].astype(jnp.float32) if fresh else acc_s[:, cols]) + term

        lax.fori_loop(0, dim // unit, tile, None)

    from_mate(WO, CW, 0)
    output(CW, 0, fresh=True)
    for t in (1, 2, 3, 4, 5):
        now = (CW, CCW) if t < 4 else (CW,) if t == 4 else ()
        before = () if t == 1 else (CW, CCW) if t < 5 else (CW,)
        for way in now:
            arrive(WO, way, t)
        for way in before:
            arrive_x(WO, way, t - 1)
        for way in now:
            from_mate(WO, way, t)
        for way in before:
            x_from_mate(WO, way, t - 1)
            output(way, t - 1)
    out_ref[...] = acc_s[:, :dim].astype(jnp.bfloat16)

    for kind in (W1, KV, WO):
        to_mate(kind, CW, 0, True).wait_send()
        for way in (CW, CCW):
            for t in range(1, STEPS[way] + 1):
                ring(kind, way, t, True).wait_send()
                to_mate(kind, way, t, True).wait_send()
                if kind != KV:
                    over_x(kind, way, t, True).wait_send()
                    x_to_mate(kind, way, t, True).wait_send()


def attend(x, gain, wq, wk, wv, wo, cos, sin):
    (tokens, dim), depth, head = x.shape, wq.shape[0], wk.shape[1]
    heads = dim // head
    anywhere, vmem = pl.BlockSpec(memory_space=pl.ANY), pl.BlockSpec(memory_space=pltpu.VMEM)
    sems = pltpu.SemaphoreType.DMA((3, 2, 5))
    return pl.pallas_call(
        functools.partial(_kernel, shift=3 * dim // 8),
        out_shape=jax.ShapeDtypeStruct((tokens, dim), jnp.bfloat16),
        in_specs=[anywhere, vmem, anywhere, anywhere, anywhere, anywhere, vmem, vmem],
        out_specs=vmem,
        scratch_shapes=[
            pltpu.VMEM((tokens, dim), jnp.bfloat16),
            pltpu.VMEM((tokens, dim), jnp.bfloat16),
            pltpu.VMEM((16 * depth, dim + 2 * head), jnp.bfloat16),
            pltpu.VMEM((16 * depth, dim), jnp.bfloat16),
            pltpu.VMEM((16 * tokens, 2 * head), jnp.bfloat16),
            pltpu.VMEM((tokens, dim + 2 * head), jnp.float32),
            pltpu.VMEM((heads * tokens, head), jnp.bfloat16),
            pltpu.VMEM((1, heads * tokens), jnp.float32),
            pltpu.VMEM((head + 8, heads * tokens), jnp.float32),
            pltpu.SemaphoreType.DMA((6,)),
            *[sems] * 8,
        ],
        compiler_params=pltpu.CompilerParams(collective_id=0, has_side_effects=True, vmem_limit_bytes=67043328),
    )(x, gain, wq, wk, wv, wo, cos, sin)


def solution(mesh):
    def step(x, gain, wq, wk, wv, wo):
        own, head = x.shape[0], wk.shape[1]
        place = lax.axis_index("sp") * own + jnp.arange(own)
        half = head // 2
        angle = place.astype(jnp.float32)[:, None] * THETA ** (-jnp.arange(half, dtype=jnp.float32) / half)
        return attend(x, gain[None], wq, wk, wv, wo, jnp.cos(angle), jnp.sin(angle))

    tokens, whole = P(("dp", "sp"), None), P("sp", None)
    return jax.shard_map(
        step,
        mesh=mesh,
        in_specs=(tokens, P(None), whole, whole, whole, whole),
        out_specs=tokens,
        check_vma=False,
    )
```

```python
import functools

import jax
import jax.numpy as jnp
from jax import lax
from jax.experimental import pallas as pl
from jax.experimental.pallas import tpu as pltpu
from jax.sharding import PartitionSpec as P

HEAD = 256
THETA = 10000
NEG = -1e30
HIDDEN = 2 * NEG
LOG2E = 1.4426950408889634
MESH = pl.DeviceIdType.MESH
CW, CCW = 0, 1
W1, KV, WO = 0, 1, 2
PIECES = 7
OWN = 7
AHEAD = {(3, 2): 0, (3, 3): 1, (4, 0): 2, (4, 1): 3}


def _dot(a, b, ca, cb):
    return lax.dot_general(a, b, (((ca,), (cb,)), ((), ())), preferred_element_type=jnp.float32)


def _chip(p):
    y = p // 4
    return 4 * y + p + y * (7 - 2 * p)


def _lane(x, unit=128):
    return x if isinstance(x, int) else pl.multiple_of(x, unit)


def _kernel(x_hbm, gain_ref, wq_hbm, wk_hbm, wv_hbm, wo_hbm, cos_ref, sin_ref, out_ref,
            x_s, a_s, w1_s, wo_s, kv_s, acc_s, q_s, top_s, mix_s,
            local, ring_send, ring_recv, x_send, x_recv, d_send, d_recv, dx_send, dx_recv, *, shift):
    tokens, dim = x_s.shape
    depth = wq_hbm.shape[0]
    head = kv_s.shape[1] // 2
    heads = dim // head
    unit = 2 * head
    half = dim // 2
    group, me = lax.axis_index("dp"), lax.axis_index("sp")
    chip, core = me // 2, me % 2
    row = chip // 4
    z = chip % 4
    place = row * 7 + z - 2 * row * z

    def device(p):
        return (group, _chip(p % 8) * 2 + core)

    right, left, twin, mate = device(place + 1), device(place + 7), (1 - group, me), (group, chip * 2 + 1 - core)

    def origin(way, t):
        return _chip((place + 8 - t) % 8 if way == CW else (place + t) % 8)

    bufs = {W1: (w1_s, depth), KV: (kv_s, tokens), WO: (wo_s, depth)}

    def whole(kind):
        return (0, bufs[kind][0].shape[1])

    def window(kind, way, t, n, of_core, cols):
        buf, rows = bufs[kind]
        begin, width = cols
        part = rows // 2
        at = (origin(way, t) * 2 + of_core) * rows + (n % 2 if way == CW else 1 - n % 2) * part
        return buf.at[pl.ds(pl.multiple_of(at, part), part), pl.ds(_lane(begin), width)]

    def ring_cols(kind):
        full = whole(kind)[1]
        return (0, full) if kind == KV else (group * shift[kind], full - shift[kind])

    def x_cols(kind, of_group):
        return (of_group * (whole(kind)[1] - shift[kind]), shift[kind])

    def copy(src, send, recv, to):
        return pltpu.make_async_remote_copy(src_ref=src, dst_ref=src, send_sem=send, recv_sem=recv, device_id=to, device_id_type=MESH)

    def ring(kind, way, n, sent):
        return copy(window(kind, way, n // 2 + (0 if sent else 1), n, core, ring_cols(kind)), ring_send.at[kind, way, n],
                    ring_recv.at[kind, way, n], right if way == CW else left)

    def over_x(kind, way, n, sent):
        return copy(window(kind, way, n // 2 + 1, n, core, x_cols(kind, group if sent else 1 - group)), x_send.at[kind, way, n],
                    x_recv.at[kind, way, n], twin)

    def to_mate(kind, way, n, sent):
        return copy(window(kind, way, n // 2 + 1, n, core if sent else 1 - core, ring_cols(kind)), d_send.at[kind, way, n],
                    d_recv.at[kind, way, n], mate)

    def x_to_mate(kind, way, n, sent):
        return copy(window(kind, way, n // 2 + 1, n, core if sent else 1 - core, x_cols(kind, 1 - group)), dx_send.at[kind, way, n],
                    dx_recv.at[kind, way, n], mate)

    def own_to_mate(kind, sent):
        buf, rows = bufs[kind]
        at = (chip * 2 + (core if sent else 1 - core)) * rows
        return copy(buf.at[pl.ds(pl.multiple_of(at, rows), rows), :], d_send.at[kind, CW, OWN], d_recv.at[kind, CW, OWN], mate)

    def begin(kind):
        for n in range(2):
            ring(kind, CW, n, True).start()
            ring(kind, CCW, n, True).start()
        own_to_mate(kind, True).start()

    def arrive(kind, n):
        for way in (CW, CCW):
            ring(kind, way, n, False).wait_recv()
            if isinstance(n, int):
                if n + 2 < PIECES:
                    ring(kind, way, n + 2, True).start()
            else:
                @pl.when(n + 2 < PIECES)
                def _():
                    ring(kind, way, n + 2, True).start()
            if kind != KV:
                over_x(kind, way, n, True).start()
            to_mate(kind, way, n, True).start()

    def arrive_x(kind, n):
        for way in (CW, CCW):
            over_x(kind, way, n, False).wait_recv()
            x_to_mate(kind, way, n, True).start()

    def pieces(t):
        return (2 * t - 2, 2 * t - 1) if t < 4 else (6,)

    def ways(t):
        return (CW, CCW) if t < 4 else (CW,)

    def from_mate(kind, t):
        for n in pieces(t):
            for way in (CW, CCW):
                to_mate(kind, way, n, False).wait_recv()

    def x_from_mate(kind, t):
        for n in pieces(t):
            for way in (CW, CCW):
                x_to_mate(kind, way, n, False).wait_recv()

    own = pl.ds(pl.multiple_of(me * depth, depth), depth)
    loads = [
        (wq_hbm.at[:, pl.ds(0, half)], w1_s.at[own, pl.ds(0, half)]),
        (wk_hbm, w1_s.at[own, pl.ds(half, head)]),
        (wv_hbm, w1_s.at[own, pl.ds(half + head, head)]),
        (wq_hbm.at[:, pl.ds(half, half)], w1_s.at[own, pl.ds(half + unit, half)]),
        (x_hbm, x_s),
        (wo_hbm, wo_s.at[own, :]),
    ]
    loads = [pltpu.make_async_copy(src, dst, local.at[i]) for i, (src, dst) in enumerate(loads)]
    for load in loads:
        load.start()
    barrier = pltpu.get_barrier_semaphore()
    for to in (right, left, twin, mate):
        pl.semaphore_signal(barrier, inc=1, device_id=to, device_id_type=MESH)
    for load in loads[:4]:
        load.wait()
    pl.semaphore_wait(barrier, 4)
    begin(W1)

    loads[4].wait()
    gain = gain_ref[...].astype(jnp.float32)[None]
    some = min(64, tokens)

    def norm(i, _):
        here = pl.ds(pl.multiple_of(i * some, some), some)
        wide = x_s[here, :].astype(jnp.float32)
        scale = lax.rsqrt(jnp.mean(wide * wide, -1, keepdims=True) + 1e-6)
        a_s[here, :] = (wide * scale * gain).astype(jnp.bfloat16)

    lax.fori_loop(0, tokens // some, norm, None)

    def project(chip_of, first, count, fresh=False):
        rows = pl.ds(pl.multiple_of(chip_of * 2 * depth, 2 * depth), 2 * depth)
        cols_a = pl.ds(pl.multiple_of(chip_of * 2 * depth, 2 * depth), 2 * depth)

        def tile(n, _):
            cols = pl.ds(pl.multiple_of((first + n) * unit, unit), unit)
            term = _dot(a_s[:, cols_a], w1_s[rows, cols], 1, 0)
            acc_s[:, cols] = term if fresh else acc_s[:, cols] + term

        lax.fori_loop(0, count, tile, None)

    mid = half // unit

    def queries(way, t):
        project(origin(way, t), 0, mid)
        project(origin(way, t), mid + 1, mid)

    own_to_mate(W1, False).wait_recv()
    project(chip, 0, 2 * mid + 1, fresh=True)

    def shared(n):
        arrive_x(W1, n)
        if n % 2 or n == 6:
            t = n // 2 + 1
            x_from_mate(W1, t)
            for way in ways(t):
                queries(way, t)

    for n in range(PIECES):
        arrive(W1, n)
        if n % 2 or n == 6:
            t = n // 2 + 1
            from_mate(W1, t)
            for way in ways(t):
                project(origin(way, t), mid, 1)
        if n >= 2:
            shared(n - 2)

    cos, sin = cos_ref[...], sin_ref[...]

    def turned(t):
        t = t.astype(jnp.bfloat16).astype(jnp.float32)
        a, b = t[:, : head // 2], t[:, head // 2 :]
        return jnp.concatenate([a * cos - b * sin, b * cos + a * sin], -1).astype(jnp.bfloat16)

    here = pl.multiple_of(me * tokens, tokens)
    kv_s[pl.ds(here, tokens), :head] = turned(acc_s[:, half : half + head])
    part = tokens // 2
    for j in range(2):
        value = acc_s[j * part : (j + 1) * part, half + head : half + unit].astype(jnp.bfloat16)
        kv_s[pl.ds(here + j * part, part), head:] = value.T if value.shape[0] == value.shape[1] else value
    begin(KV)

    shared(5)
    shared(6)

    def turn(h, _):
        cols = pl.ds(pl.multiple_of(h * head + (h // (heads // 2)) * unit, head), head)
        q_s[pl.ds(pl.multiple_of(h * tokens, tokens), tokens), :] = turned(acc_s[:, cols])

    lax.fori_loop(0, heads, turn, None)

    e = head**-0.5 * LOG2E
    top_s[...] = jnp.full(top_s.shape, NEG, jnp.float32)
    mix_s[...] = jnp.zeros(mix_s.shape, jnp.float32)

    def block(of, masked):
        base = pl.multiple_of(of * tokens, tokens)
        keys = kv_s[pl.ds(base, tokens), :head]
        scores = [_dot(keys, q_s[h * tokens : (h + 1) * tokens, :], 1, 1) for h in range(heads)]
        ok = None
        if masked:
            ok = lax.broadcasted_iota(jnp.int32, (tokens, tokens), 0) <= lax.broadcasted_iota(jnp.int32, (tokens, tokens), 1)
        weights, keeps = [], []
        for h, s in enumerate(scores):
            at = slice(h * tokens, (h + 1) * tokens)
            if masked:
                s = jnp.where(ok, s, HIDDEN)
            old = top_s[:, at]
            top = jnp.maximum(old, s.max(axis=0, keepdims=True))
            top_s[:, at] = top
            weights.append(jnp.exp2((s - top) * e).astype(jnp.bfloat16))
            keeps.append(jnp.exp2((old - top) * e))
        values = jnp.concatenate([kv_s[pl.ds(base + j * part, part), head:] for j in range(2)], axis=1)
        values = jnp.concatenate([values, jnp.ones((8, tokens), jnp.bfloat16)], axis=0)
        for h, (p, keep) in enumerate(zip(weights, keeps)):
            at = slice(h * tokens, (h + 1) * tokens)
            mix_s[:, at] = mix_s[:, at] * keep + _dot(values, p, 1, 0)

    block(me, True)
    own_to_mate(KV, False).wait_recv()
    arrive(KV, 0)

    def step(t, _):
        @pl.when((t > 0) & (t < 4))
        def _():
            arrive(KV, 2 * t - 1)

        def one(j, _):
            way, other = j // 2, j % 2

            @pl.when((t > 0) & (t < 4) & (j == 2))
            def _():
                arrive(KV, 2 * t)

            @pl.when((t == 2) & (j == 2))
            def _():
                loads[5].wait()
                begin(WO)

            for slot, n in AHEAD.items():
                @pl.when((t == slot[0]) & (j == slot[1]))
                def _():
                    arrive(WO, n)

            @pl.when((t > 0) & (t < 4) & (j == 1))
            def _():
                for way in (CW, CCW):
                    for i in range(2):
                        to_mate(KV, way, 2 * t - 2 + i, False).wait_recv()

            @pl.when((t == 4) & (j == 1))
            def _():
                for way in (CW, CCW):
                    to_mate(KV, way, 6, False).wait_recv()

            there = (place + (8 - t) * (1 - way) + t * way) % 8
            of = _chip(there) * 2 + (1 - other) * core + other * (1 - core)

            @pl.when((of < me) & ((way == 0) | ((t > 0) & (t < 4))))
            def _():
                block(of, False)

        lax.fori_loop(0, 4, one, None)

    lax.fori_loop(0, 5, step, None)

    def finish(h, _):
        at = pl.ds(pl.multiple_of(h * tokens, tokens), tokens)
        total = mix_s[head : head + 1, at]
        a_s[:, pl.ds(pl.multiple_of(h * head, head), head)] = (mix_s[:head, at] * (1 / total)).T.astype(jnp.bfloat16)

    lax.fori_loop(0, heads, finish, None)

    def output(way, t, fresh=False):
        chip_of = origin(way, t)
        rows = pl.ds(pl.multiple_of(chip_of * 2 * depth, 2 * depth), 2 * depth)

        def tile(n, _):
            cols = pl.ds(pl.multiple_of(n * unit, unit), unit)
            term = _dot(a_s[:, rows], wo_s[rows, cols], 1, 0)
            acc_s[:, cols] = (x_s[:, cols].astype(jnp.float32) if fresh else acc_s[:, cols]) + term

        lax.fori_loop(0, dim // unit, tile, None)

    own_to_mate(WO, False).wait_recv()
    output(CW, 0, fresh=True)
    done = len(AHEAD)
    for n in range(min(done, 2), PIECES + 2):
        if done <= n < PIECES:
            arrive(WO, n)
        m = n - 2
        if m >= 0:
            arrive_x(WO, m)
            if m % 2 or m == 6:
                t = m // 2 + 1
                from_mate(WO, t)
                x_from_mate(WO, t)
                for way in ways(t):
                    output(way, t)
    out_ref[...] = acc_s[:, :dim].astype(jnp.bfloat16)

    for kind in (W1, KV, WO):
        own_to_mate(kind, True).wait_send()
        for way in (CW, CCW):
            for n in range(PIECES):
                ring(kind, way, n, True).wait_send()
                to_mate(kind, way, n, True).wait_send()
                if kind != KV:
                    over_x(kind, way, n, True).wait_send()
                    x_to_mate(kind, way, n, True).wait_send()


def attend(x, gain, wq, wk, wv, wo, cos, sin):
    (tokens, dim), depth, head = x.shape, wq.shape[0], wk.shape[1]
    heads = dim // head
    anywhere, vmem = pl.BlockSpec(memory_space=pl.ANY), pl.BlockSpec(memory_space=pltpu.VMEM)
    sems = pltpu.SemaphoreType.DMA((3, 2, 8))
    return pl.pallas_call(
        functools.partial(_kernel, shift={W1: 3 * dim // 8, WO: 3 * dim // 8}),
        out_shape=jax.ShapeDtypeStruct((tokens, dim), jnp.bfloat16),
        in_specs=[anywhere, vmem, anywhere, anywhere, anywhere, anywhere, vmem, vmem],
        out_specs=vmem,
        scratch_shapes=[
            pltpu.VMEM((tokens, dim), jnp.bfloat16),
            pltpu.VMEM((tokens, dim), jnp.bfloat16),
            pltpu.VMEM((16 * depth, dim + 2 * head), jnp.bfloat16),
            pltpu.VMEM((16 * depth, dim), jnp.bfloat16),
            pltpu.VMEM((16 * tokens, 2 * head), jnp.bfloat16),
            pltpu.VMEM((tokens, dim + 2 * head), jnp.float32),
            pltpu.VMEM((heads * tokens, head), jnp.bfloat16),
            pltpu.VMEM((1, heads * tokens), jnp.float32),
            pltpu.VMEM((head + 8, heads * tokens), jnp.float32),
            pltpu.SemaphoreType.DMA((6,)),
            *[sems] * 8,
        ],
        compiler_params=pltpu.CompilerParams(collective_id=0, has_side_effects=True, vmem_limit_bytes=67043328),
    )(x, gain, wq, wk, wv, wo, cos, sin)


def solution(mesh):
    def step(x, gain, wq, wk, wv, wo):
        own, head = x.shape[0], wk.shape[1]
        place = lax.axis_index("sp") * own + jnp.arange(own)
        half = head // 2
        angle = place.astype(jnp.float32)[:, None] * THETA ** (-jnp.arange(half, dtype=jnp.float32) / half)
        return attend(x, gain, wq, wk, wv, wo, jnp.cos(angle), jnp.sin(angle))

    tokens, whole = P(("dp", "sp"), None), P("sp", None)
    return jax.shard_map(
        step,
        mesh=mesh,
        in_specs=(tokens, P(None), whole, whole, whole, whole),
        out_specs=tokens,
        check_vma=False,
    )
```

```python
import functools

import jax
import jax.numpy as jnp
from jax import lax
from jax.experimental import pallas as pl
from jax.experimental.pallas import tpu as pltpu
from jax.sharding import PartitionSpec as P

HEAD = 256
THETA = 10000
NEG = -1e30
HIDDEN = 2 * NEG
LOG2E = 1.4426950408889634
MESH = pl.DeviceIdType.MESH
CW, CCW = 0, 1
W1, KV, WO, X = 0, 1, 2, 3
PIECES = 7
RELAYS = (
    ((1, 0), KV, 1), ((1, 2), KV, 2), ((1, 3), KV, 3), ((1, 3), WO, -1), ((2, 1), KV, 4), ((2, 2), KV, 5), ((2, 3), WO, 0), ((3, 0), WO, 1), ((3, 1), X, 0),
    ((3, 2), KV, 6), ((3, 2), WO, 2), ((3, 2), X, 1), ((3, 3), WO, 3), ((4, 0), WO, 4), ((4, 0), X, 2), ((4, 1), WO, 5), ((4, 1), X, 3),
)


def _dot(a, b, ca, cb):
    return lax.dot_general(a, b, (((ca,), (cb,)), ((), ())), preferred_element_type=jnp.float32)


def _chip(p):
    y = p // 4
    return 4 * y + p + y * (7 - 2 * p)


def _lane(x, unit=128):
    return x if isinstance(x, int) else pl.multiple_of(x, unit)


def _kernel(x_hbm, gain_ref, rate_ref, wq_hbm, wk_hbm, wv_hbm, wo_hbm, out_hbm,
            cos_s, sin_s, x_s, a_s, w1_s, wo_s, kv_s, acc_s, q_s, top_s, mix_s,
            local, ring_send, ring_recv, x_send, x_recv, own_send, d_send, d_recv, dx_send, dx_recv, *, shift):
    tokens, dim = x_s.shape
    depth = wq_hbm.shape[0]
    head = kv_s.shape[1] // 2
    heads = dim // head
    unit = 2 * head
    half = dim // 2
    group, me = lax.axis_index("dp"), lax.axis_index("sp")
    chip, core = me // 2, me % 2
    row = chip // 4
    z = chip % 4
    place = row * 7 + z - 2 * row * z

    def device(p):
        return (group, _chip(p % 8) * 2 + core)

    right, left, twin, mate = device(place + 1), device(place + 7), (1 - group, me), (group, chip * 2 + 1 - core)

    def origin(way, t):
        return _chip((place + 8 - t) % 8 if way == CW else (place + t) % 8)

    bufs = {W1: (w1_s, depth), KV: (kv_s, tokens), WO: (wo_s, depth)}

    def whole(kind):
        return (0, bufs[kind][0].shape[1])

    def window(kind, way, t, n, of_core, cols):
        buf, rows = bufs[kind]
        begin, width = cols
        part = rows // 2
        at = (origin(way, t) * 2 + of_core) * rows + (n % 2 if way == CW else 1 - n % 2) * part
        return buf.at[pl.ds(pl.multiple_of(at, part), part), pl.ds(_lane(begin), width)]

    def ring_cols(kind):
        full = whole(kind)[1]
        return (0, full) if kind == KV else (group * shift[kind], full - shift[kind])

    def x_cols(kind, of_group):
        return (of_group * (whole(kind)[1] - shift[kind]), shift[kind])

    def x_pieces(kind):
        return 0 if kind == KV else PIECES

    def copy(src, send, recv, to):
        return pltpu.make_async_remote_copy(src_ref=src, dst_ref=src, send_sem=send, recv_sem=recv, device_id=to, device_id_type=MESH)

    def ring(kind, way, n, sent):
        return copy(window(kind, way, n // 2 + (0 if sent else 1), n, core, ring_cols(kind)), ring_send.at[kind], ring_recv.at[kind, way, n],
                    right if way == CW else left)

    def over_x(kind, way, n, sent):
        return copy(window(kind, way, n // 2 + 1, n, core, x_cols(kind, group if sent else 1 - group)), x_send.at[kind // 2],
                    x_recv.at[kind // 2, way, n], twin)

    def to_mate(kind, way, n):
        return copy(window(kind, way, n // 2 + 1, n, core, ring_cols(kind)), d_send.at[kind], d_recv.at[kind, n // 2 + 1], mate)

    def x_to_mate(kind, way, n):
        return copy(window(kind, way, n // 2 + 1, n, core, x_cols(kind, 1 - group)), dx_send.at[kind // 2], dx_recv.at[kind // 2, n // 2 + 1], mate)

    def own_to_mate(kind, sent):
        buf, rows = bufs[kind]
        at = (chip * 2 + (core if sent else 1 - core)) * rows
        return copy(buf.at[pl.ds(pl.multiple_of(at, rows), rows), :], own_send.at[kind], d_recv.at[kind, 0], mate)

    def bulk(kind, count, cols, send, recv):
        buf, rows = bufs[kind]
        begin, width = cols
        return copy(buf.at[pl.ds(0, count * (rows // 2)), pl.ds(_lane(begin), width)], send, recv, mate)

    def begin(kind):
        for n in range(2):
            ring(kind, CW, n, True).start()
            ring(kind, CCW, n, True).start()
        own_to_mate(kind, True).start()

    def arrive(kind, n):
        for way in (CW, CCW):
            ring(kind, way, n, False).wait_recv()
            if isinstance(n, int):
                if n + 2 < PIECES:
                    ring(kind, way, n + 2, True).start()
            else:
                @pl.when(n + 2 < PIECES)
                def _():
                    ring(kind, way, n + 2, True).start()
            if n < x_pieces(kind):
                over_x(kind, way, n, True).start()
            to_mate(kind, way, n).start()

    def arrive_x(kind, n):
        for way in (CW, CCW):
            over_x(kind, way, n, False).wait_recv()
            x_to_mate(kind, way, n).start()

    def ways(t):
        return (CW, CCW) if t < 4 else (CW,)

    def from_mate(kind, t):
        count = 4 if not isinstance(t, int) or t < 4 else 2
        bulk(kind, count, ring_cols(kind), d_send.at[kind], d_recv.at[kind, t]).wait_recv()

    def x_from_mate(kind, t):
        bulk(kind, 4 if t < 4 else 2, x_cols(kind, 1 - group), dx_send.at[kind // 2], dx_recv.at[kind // 2, t]).wait_recv()

    own = pl.ds(pl.multiple_of(me * depth, depth), depth)
    loads = [
        (wq_hbm.at[:, pl.ds(0, half)], w1_s.at[own, pl.ds(0, half)]),
        (wk_hbm, w1_s.at[own, pl.ds(half, head)]),
        (wv_hbm, w1_s.at[own, pl.ds(half + head, head)]),
        (wq_hbm.at[:, pl.ds(half, half)], w1_s.at[own, pl.ds(half + unit, half)]),
        (x_hbm, x_s),
        (wo_hbm, wo_s.at[own, :]),
    ]
    loads = [pltpu.make_async_copy(src, dst, local.at[i]) for i, (src, dst) in enumerate(loads)]
    for load in loads:
        load.start()
    barrier = pltpu.get_barrier_semaphore()
    for to in (right, left, twin, mate):
        pl.semaphore_signal(barrier, inc=1, device_id=to, device_id_type=MESH)
    for load in loads[:4]:
        load.wait()
    pl.semaphore_wait(barrier, 4)
    begin(W1)

    loads[4].wait()
    gain = gain_ref[...].astype(jnp.float32)[None]
    some = min(64, tokens)

    def norm(i, _):
        here = pl.ds(pl.multiple_of(i * some, some), some)
        wide = x_s[here, :].astype(jnp.float32)
        scale = lax.rsqrt(jnp.mean(wide * wide, -1, keepdims=True) + 1e-6)
        a_s[here, :] = (wide * scale * gain).astype(jnp.bfloat16)

    lax.fori_loop(0, tokens // some, norm, None)
    spot = (me * tokens + lax.broadcasted_iota(jnp.int32, (tokens, head // 2), 0)).astype(jnp.float32)
    angle = spot * rate_ref[...]
    cos_s[...] = jnp.cos(angle)
    sin_s[...] = jnp.sin(angle)

    def project(chip_of, first, count, fresh=False):
        rows = pl.ds(pl.multiple_of(chip_of * 2 * depth, 2 * depth), 2 * depth)
        cols_a = pl.ds(pl.multiple_of(chip_of * 2 * depth, 2 * depth), 2 * depth)

        def tile(n, _):
            cols = pl.ds(pl.multiple_of((first + n) * unit, unit), unit)
            term = _dot(a_s[:, cols_a], w1_s[rows, cols], 1, 0)
            acc_s[:, cols] = term if fresh else acc_s[:, cols] + term

        lax.fori_loop(0, count, tile, None)

    mid = half // unit

    own_to_mate(W1, False).wait_recv()
    project(chip, 0, 2 * mid + 1, fresh=True)

    def shared(t):
        x_from_mate(W1, t)
        for way in ways(t):
            project(origin(way, t), (1 - group) * (mid + 1), mid)

    def carried(t):
        from_mate(W1, t)
        for way in ways(t):
            project(origin(way, t), group * mid, mid + 1)

    for n in range(PIECES):
        arrive(W1, n)
        if n in (2, 4):
            carried(n // 2)
        if n == 4:
            shared(1)
        if 2 <= n < 6:
            arrive_x(W1, n - 2)
        if n == 5:
            carried(3)
    carried(4)


    cos, sin = cos_s[...], sin_s[...]

    def turned(t):
        t = t.astype(jnp.bfloat16).astype(jnp.float32)
        a, b = t[:, : head // 2], t[:, head // 2 :]
        return jnp.concatenate([a * cos - b * sin, b * cos + a * sin], -1).astype(jnp.bfloat16)

    here = pl.multiple_of(me * tokens, tokens)
    kv_s[pl.ds(here, tokens), :head] = turned(acc_s[:, half : half + head])
    part = tokens // 2
    for j in range(2):
        value = acc_s[j * part : (j + 1) * part, half + head : half + unit].astype(jnp.bfloat16)
        kv_s[pl.ds(here + j * part, part), head:] = value.T if value.shape[0] == value.shape[1] else value
    begin(KV)
    arrive_x(W1, 4)
    shared(2)
    arrive_x(W1, 5)

    def head_of(i):
        return (i + group * (heads // 2)) % heads

    def turn(i, _):
        h = head_of(i)
        cols = pl.ds(pl.multiple_of(h * head + (h // (heads // 2)) * unit, head), head)
        q_s[pl.ds(pl.multiple_of(i * tokens, tokens), tokens), :] = turned(acc_s[:, cols])

    e = head**-0.5 * LOG2E
    top_s[...] = jnp.full(top_s.shape, NEG, jnp.float32)
    mix_s[...] = jnp.zeros(mix_s.shape, jnp.float32)

    few = heads // 2

    def block(first, count, masked, begin):
        base = pl.multiple_of(first * tokens, tokens)
        at = [pl.ds(pl.multiple_of((begin + i) * tokens, tokens), tokens) for i in range(few)]
        keys = kv_s[pl.ds(base, count * tokens), :head]
        scores = [_dot(keys, q_s[at[i], :], 1, 1) for i in range(few)]
        if masked:
            ok = lax.broadcasted_iota(jnp.int32, (tokens, tokens), 0) <= lax.broadcasted_iota(jnp.int32, (tokens, tokens), 1)
            scores = [jnp.where(ok, s, HIDDEN) for s in scores]
        weights, keeps = [], []
        for i, s in enumerate(scores):
            old = top_s[:, at[i]]
            top = jnp.maximum(old, s.max(axis=0, keepdims=True))
            top_s[:, at[i]] = top
            weights.append(jnp.exp2((s - top) * e).astype(jnp.bfloat16))
            keeps.append(jnp.exp2((old - top) * e))
        values = jnp.concatenate([kv_s[pl.ds(base + j * part, part), head:] for j in range(2 * count)], axis=1)
        values = jnp.concatenate([values, jnp.ones((8, count * tokens), jnp.bfloat16)], axis=0)
        for i in range(few):
            mix_s[:, at[i]] = mix_s[:, at[i]] * keeps[i] + _dot(values, weights[i], 1, 0)

    for which in (0, 1):
        if which == 1:
            arrive_x(W1, 6)
            shared(3)
            shared(4)
            arrive(KV, 0)
        lax.fori_loop(which * few, (which + 1) * few, turn, None)
        block(me, 1, True, which * few)
        if which == 0:
            own_to_mate(KV, False).wait_recv()

        @pl.when(core == 1)
        def _():
            block(me - 1, 1, False, which * few)

    def step(t, _):
        def one(j, _):
            way, which = j // 2, j % 2

            for slot in sorted({slot for slot, _, _ in RELAYS}):
                @pl.when((t == slot[0]) & (j == slot[1]))
                def _():
                    for kind, n in (entry[1:] for entry in RELAYS if entry[0] == slot):
                        if n < 0:
                            loads[5].wait()
                            begin(kind)
                        elif kind == X:
                            arrive_x(WO, n)
                        else:
                            arrive(kind, n)

            @pl.when((t < 4) & (j == 0))
            def _():
                from_mate(KV, t)

            @pl.when((t == 4) & (j == 0))
            def _():
                from_mate(KV, 4)

            of = _chip((place + (8 - t) * (1 - way) + t * way) % 8)

            @pl.when((of < chip) & ((way == 0) | (t < 4)))
            def _():
                block(of * 2, 2, False, which * few)

        lax.fori_loop(0, 4, one, None)

    lax.fori_loop(1, 5, step, None)

    def finish(h, _):
        at = pl.ds(pl.multiple_of(h * tokens, tokens), tokens)
        total = mix_s[head : head + 1, at]
        a_s[:, pl.ds(pl.multiple_of(head_of(h) * head, head), head)] = (mix_s[:head, at] * (1 / total)).T.astype(jnp.bfloat16)

    lax.fori_loop(0, heads, finish, None)

    def store(n):
        cols = pl.ds(pl.multiple_of(n * unit, unit), unit)
        return pltpu.make_async_copy(x_s.at[:, cols], out_hbm.at[:, cols], local.at[6 + n])

    def output(chips, fresh=False, last=False):
        rows = [pl.ds(pl.multiple_of(c * 2 * depth, 2 * depth), 2 * depth) for c in chips]

        def tile(n, _):
            cols = pl.ds(pl.multiple_of(n * unit, unit), unit)
            total = x_s[:, cols].astype(jnp.float32) if fresh else acc_s[:, cols]
            total += functools.reduce(jnp.add, [_dot(a_s[:, r], wo_s[r, cols], 1, 0) for r in rows])
            if last:
                x_s[:, cols] = total.astype(jnp.bfloat16)
                store(n).start()
            else:
                acc_s[:, cols] = total

        lax.fori_loop(0, dim // unit, tile, None)

    own_to_mate(WO, False).wait_recv()
    done, done_x = (sum(kind == k and n >= 0 for _, kind, n in RELAYS) for k in (WO, X))
    begun = min(done, done_x)
    t = 1
    for n in range(begun - 1, PIECES):
        if n >= done:
            arrive(WO, n)
        if done_x <= n < x_pieces(WO):
            arrive_x(WO, n)
        while t < 4 and 2 * t - 1 <= n - (n >= begun):
            from_mate(WO, t)
            x_from_mate(WO, t)
            output([*([chip] if t == 1 else []), *(origin(way, t) for way in ways(t))], fresh=t == 1)
            t += 1
    from_mate(WO, 4)
    x_from_mate(WO, 4)
    output([origin(CW, 4)], last=True)

    for kind in (W1, KV, WO):
        own_to_mate(kind, True).wait_send()
        bulk(kind, 2 * PIECES, ring_cols(kind), ring_send.at[kind], d_recv.at[kind, 0]).wait_send()
        bulk(kind, 2 * PIECES, ring_cols(kind), d_send.at[kind], d_recv.at[kind, 0]).wait_send()
        if kind != KV:
            bulk(kind, 2 * x_pieces(kind), x_cols(kind, group), x_send.at[kind // 2], d_recv.at[kind, 0]).wait_send()
            bulk(kind, 2 * x_pieces(kind), x_cols(kind, 1 - group), dx_send.at[kind // 2], d_recv.at[kind, 0]).wait_send()
    for n in range(dim // unit):
        store(n).wait()


def attend(x, gain, wq, wk, wv, wo):
    half = wk.shape[1] // 2
    rate = THETA ** (-jnp.arange(half, dtype=jnp.float32) / half)
    (tokens, dim), depth, head = x.shape, wq.shape[0], wk.shape[1]
    heads = dim // head
    anywhere, vmem = pl.BlockSpec(memory_space=pl.ANY), pl.BlockSpec(memory_space=pltpu.VMEM)
    return pl.pallas_call(
        functools.partial(_kernel, shift={W1: 8 * dim // 16, WO: 6 * dim // 16}),
        out_shape=jax.ShapeDtypeStruct((tokens, dim), jnp.bfloat16),
        in_specs=[anywhere, vmem, vmem, anywhere, anywhere, anywhere, anywhere],
        out_specs=anywhere,
        scratch_shapes=[
            *[pltpu.VMEM((tokens, head // 2), jnp.float32)] * 2,
            pltpu.VMEM((tokens, dim), jnp.bfloat16),
            pltpu.VMEM((tokens, dim), jnp.bfloat16),
            pltpu.VMEM((16 * depth, dim + 2 * head), jnp.bfloat16),
            pltpu.VMEM((16 * depth, dim), jnp.bfloat16),
            pltpu.VMEM((16 * tokens, 2 * head), jnp.bfloat16),
            pltpu.VMEM((tokens, dim + 2 * head), jnp.float32),
            pltpu.VMEM((heads * tokens, head), jnp.bfloat16),
            pltpu.VMEM((1, heads * tokens), jnp.float32),
            pltpu.VMEM((head + 8, heads * tokens), jnp.float32),
            pltpu.SemaphoreType.DMA((10,)),
            *[pltpu.SemaphoreType.DMA(n) for n in ((3,), (3, 2, PIECES), (2,), (2, 2, PIECES), (3,), (3,), (3, 5), (2,), (2, 5))],
        ],
        compiler_params=pltpu.CompilerParams(collective_id=0, has_side_effects=True, vmem_limit_bytes=67043328),
    )(x, gain, rate[None], wq, wk, wv, wo)


def solution(mesh):
    tokens, whole = P(("dp", "sp"), None), P("sp", None)
    return jax.shard_map(
        attend,
        mesh=mesh,
        in_specs=(tokens, P(None), whole, whole, whole, whole),
        out_specs=tokens,
        check_vma=False,
    )
```

```python
import functools

import jax
import jax.numpy as jnp
from jax import lax
from jax.experimental import pallas as pl
from jax.experimental.pallas import tpu as pltpu
from jax.sharding import PartitionSpec as P

HEAD = 256
THETA = 10000
NEG = -1e30
HIDDEN = 2 * NEG
LOG2E = 1.4426950408889634
MESH = pl.DeviceIdType.MESH
CW, CCW = 0, 1
W1, KV, WO, X, ON = 0, 1, 2, 3, 4
PIECES = 7
RELAYS = (
    ((1, 0), KV, 1), ((1, 0), WO, -1), ((1, 2), KV, 2), ((1, 3), KV, 3), ((2, 0), ON, 2), ((2, 0), X, 0), ((2, 1), WO, 1), ((2, 1), ON, 3), ((2, 1), KV, 4),
    ((2, 3), KV, 5), ((3, 0), WO, 2), ((3, 0), ON, 4), ((3, 0), X, 1), ((3, 1), WO, 3), ((3, 1), ON, 5), ((3, 2), KV, 6), ((3, 3), X, 2), ((4, 0), WO, 4),
    ((4, 0), ON, 6), ((4, 1), WO, 5), ((4, 1), X, 3),
)


def _dot(a, b, ca, cb):
    return lax.dot_general(a, b, (((ca,), (cb,)), ((), ())), preferred_element_type=jnp.float32)


def _chip(p):
    y = p // 4
    return 4 * y + p + y * (7 - 2 * p)


def _lane(x, unit=128):
    return x if isinstance(x, int) else pl.multiple_of(x, unit)


def _kernel(x_hbm, gain_ref, rate_ref, wq_hbm, wk_hbm, wv_hbm, wo_hbm, out_hbm,
            cos_s, sin_s, x_s, a_s, w1_s, wo_s, kv_s, acc_s, q_s, top_s, mix_s,
            local, ring_send, ring_recv, x_send, x_recv, own_send, d_send, d_recv, dx_send, dx_recv, *, shift):
    tokens, dim = x_s.shape
    depth = wq_hbm.shape[0]
    head = kv_s.shape[1] // 2
    heads = dim // head
    unit = 2 * head
    half = dim // 2
    group, me = lax.axis_index("dp"), lax.axis_index("sp")
    chip, core = me // 2, me % 2
    row = chip // 4
    z = chip % 4
    place = row * 7 + z - 2 * row * z

    def device(p):
        return (group, _chip(p % 8) * 2 + core)

    right, left, twin, mate = device(place + 1), device(place + 7), (1 - group, me), (group, chip * 2 + 1 - core)

    def origin(way, t):
        return _chip((place + 8 - t) % 8 if way == CW else (place + t) % 8)

    bufs = {W1: (w1_s, depth), KV: (kv_s, tokens), WO: (wo_s, depth)}

    def whole(kind):
        return (0, bufs[kind][0].shape[1])

    def window(kind, way, t, n, of_core, cols):
        buf, rows = bufs[kind]
        begin, width = cols
        part = rows // 2
        at = (origin(way, t) * 2 + of_core) * rows + (n % 2 if way == CW else 1 - n % 2) * part
        return buf.at[pl.ds(pl.multiple_of(at, part), part), pl.ds(_lane(begin), width)]

    def ring_cols(kind):
        full = whole(kind)[1]
        return (0, full) if kind == KV else (group * shift[kind], full - shift[kind])

    def x_cols(kind, of_group):
        return (of_group * (whole(kind)[1] - shift[kind]), shift[kind])

    def x_pieces(kind):
        return 0 if kind == KV else PIECES

    def copy(src, send, recv, to):
        return pltpu.make_async_remote_copy(src_ref=src, dst_ref=src, send_sem=send, recv_sem=recv, device_id=to, device_id_type=MESH)

    def ring(kind, way, n, sent):
        return copy(window(kind, way, n // 2 + (0 if sent else 1), n, core, ring_cols(kind)), ring_send.at[kind], ring_recv.at[kind, way, n],
                    right if way == CW else left)

    def over_x(kind, way, n, sent):
        return copy(window(kind, way, n // 2 + 1, n, core, x_cols(kind, group if sent else 1 - group)), x_send.at[kind // 2],
                    x_recv.at[kind // 2, way, n], twin)

    def to_mate(kind, way, n):
        return copy(window(kind, way, n // 2 + 1, n, core, ring_cols(kind)), d_send.at[kind], d_recv.at[kind, n // 2 + 1], mate)

    def x_to_mate(kind, way, n):
        return copy(window(kind, way, n // 2 + 1, n, core, x_cols(kind, 1 - group)), dx_send.at[kind // 2], dx_recv.at[kind // 2, n // 2 + 1], mate)

    def own_to_mate(kind, sent):
        buf, rows = bufs[kind]
        at = (chip * 2 + (core if sent else 1 - core)) * rows
        return copy(buf.at[pl.ds(pl.multiple_of(at, rows), rows), :], own_send.at[kind], d_recv.at[kind, 0], mate)

    def bulk(kind, count, cols, send, recv):
        buf, rows = bufs[kind]
        begin, width = cols
        return copy(buf.at[pl.ds(0, count * (rows // 2)), pl.ds(_lane(begin), width)], send, recv, mate)

    def begin(kind, pieces=(0, 1)):
        for n in pieces:
            ring(kind, CW, n, True).start()
            ring(kind, CCW, n, True).start()
        if pieces[0] == 0:
            own_to_mate(kind, True).start()

    def forward(kind, n):
        for way in (CW, CCW):
            ring(kind, way, n, True).start()

    def arrive(kind, n, onward=True):
        for way in (CW, CCW):
            ring(kind, way, n, False).wait_recv()
            if onward and n + 2 < PIECES:
                ring(kind, way, n + 2, True).start()
            if kind != KV:
                over_x(kind, way, n, True).start()
            to_mate(kind, way, n).start()

    def arrive_x(kind, n):
        for way in (CW, CCW):
            over_x(kind, way, n, False).wait_recv()
            x_to_mate(kind, way, n).start()

    def ways(t):
        return (CW, CCW) if t < 4 else (CW,)

    def from_mate(kind, t):
        count = 4 if not isinstance(t, int) or t < 4 else 2
        bulk(kind, count, ring_cols(kind), d_send.at[kind], d_recv.at[kind, t]).wait_recv()

    def x_from_mate(kind, t):
        bulk(kind, 4 if t < 4 else 2, x_cols(kind, 1 - group), dx_send.at[kind // 2], dx_recv.at[kind // 2, t]).wait_recv()

    own = pl.ds(pl.multiple_of(me * depth, depth), depth)
    loads = [
        (wq_hbm.at[:, pl.ds(0, half)], w1_s.at[own, pl.ds(0, half)]),
        (wk_hbm, w1_s.at[own, pl.ds(half, head)]),
        (wv_hbm, w1_s.at[own, pl.ds(half + head, head)]),
        (wq_hbm.at[:, pl.ds(half, half)], w1_s.at[own, pl.ds(half + unit, half)]),
        (x_hbm, x_s),
        (wo_hbm, wo_s.at[own, :]),
    ]
    loads = [pltpu.make_async_copy(src, dst, local.at[i]) for i, (src, dst) in enumerate(loads)]
    for load in loads:
        load.start()
    barrier = pltpu.get_barrier_semaphore()
    for to in (right, left, twin, mate):
        pl.semaphore_signal(barrier, inc=1, device_id=to, device_id_type=MESH)
    for load in loads[:4]:
        load.wait()
    pl.semaphore_wait(barrier, 4)
    begin(W1)

    loads[4].wait()
    gain = gain_ref[...].astype(jnp.float32)[None]
    some = min(64, tokens)

    def norm(i, _):
        here = pl.ds(pl.multiple_of(i * some, some), some)
        wide = x_s[here, :].astype(jnp.float32)
        scale = lax.rsqrt(jnp.mean(wide * wide, -1, keepdims=True) + 1e-6)
        a_s[here, :] = (wide * scale * gain).astype(jnp.bfloat16)

    lax.fori_loop(0, tokens // some, norm, None)
    spot = (me * tokens + lax.broadcasted_iota(jnp.int32, (tokens, head // 2), 0)).astype(jnp.float32)
    angle = spot * rate_ref[...]
    cos_s[...] = jnp.cos(angle)
    sin_s[...] = jnp.sin(angle)

    def project(chip_of, first, count, fresh=False):
        rows = pl.ds(pl.multiple_of(chip_of * 2 * depth, 2 * depth), 2 * depth)
        cols_a = pl.ds(pl.multiple_of(chip_of * 2 * depth, 2 * depth), 2 * depth)

        def tile(n, _):
            cols = pl.ds(pl.multiple_of((first + n) * unit, unit), unit)
            term = _dot(a_s[:, cols_a], w1_s[rows, cols], 1, 0)
            acc_s[:, cols] = term if fresh else acc_s[:, cols] + term

        lax.fori_loop(0, count, tile, None)

    mid = half // unit

    own_to_mate(W1, False).wait_recv()
    project(chip, 0, 2 * mid + 1, fresh=True)

    def shared(t):
        x_from_mate(W1, t)
        for way in ways(t):
            project(origin(way, t), (1 - group) * (mid + 1), mid)

    def carried(t):
        from_mate(W1, t)
        for way in ways(t):
            project(origin(way, t), group * mid, mid + 1)

    for n in range(PIECES):
        arrive(W1, n)
        if n == 5:
            loads[5].wait()
            begin(WO, (0,))
        if n % 2 == 0 and n:
            carried(n // 2)
        if n == 4:
            shared(1)
        if 2 <= n < 6:
            arrive_x(W1, n - 2)
    carried(4)


    cos, sin = cos_s[...], sin_s[...]

    def turned(t):
        t = t.astype(jnp.bfloat16).astype(jnp.float32)
        a, b = t[:, : head // 2], t[:, head // 2 :]
        return jnp.concatenate([a * cos - b * sin, b * cos + a * sin], -1).astype(jnp.bfloat16)

    here = pl.multiple_of(me * tokens, tokens)
    kv_s[pl.ds(here, tokens), :head] = turned(acc_s[:, half : half + head])
    part = tokens // 2
    for j in range(2):
        value = acc_s[j * part : (j + 1) * part, half + head : half + unit].astype(jnp.bfloat16)
        kv_s[pl.ds(here + j * part, part), head:] = value.T if value.shape[0] == value.shape[1] else value
    begin(KV)
    arrive_x(W1, 4)
    shared(2)

    def head_of(i):
        return (i + group * (heads // 2)) % heads

    def turn(i, _):
        h = head_of(i)
        cols = pl.ds(pl.multiple_of(h * head + (h // (heads // 2)) * unit, head), head)
        q_s[pl.ds(pl.multiple_of(i * tokens, tokens), tokens), :] = turned(acc_s[:, cols])

    e = head**-0.5 * LOG2E
    top_s[...] = jnp.full(top_s.shape, NEG, jnp.float32)
    mix_s[...] = jnp.zeros(mix_s.shape, jnp.float32)

    few = heads // 2

    def block(first, count, masked, begin):
        base = pl.multiple_of(first * tokens, tokens)
        at = [pl.ds(pl.multiple_of((begin + i) * tokens, tokens), tokens) for i in range(few)]
        keys = kv_s[pl.ds(base, count * tokens), :head]
        scores = [_dot(keys, q_s[at[i], :], 1, 1) for i in range(few)]
        if masked:
            ok = lax.broadcasted_iota(jnp.int32, (tokens, tokens), 0) <= lax.broadcasted_iota(jnp.int32, (tokens, tokens), 1)
            scores = [jnp.where(ok, s, HIDDEN) for s in scores]
        weights, keeps = [], []
        for i, s in enumerate(scores):
            old = top_s[:, at[i]]
            top = jnp.maximum(old, s.max(axis=0, keepdims=True))
            top_s[:, at[i]] = top
            weights.append(jnp.exp2((s - top) * e).astype(jnp.bfloat16))
            keeps.append(jnp.exp2((old - top) * e))
        values = jnp.concatenate([kv_s[pl.ds(base + j * part, part), head:] for j in range(2 * count)], axis=1)
        values = jnp.concatenate([values, jnp.ones((8, count * tokens), jnp.bfloat16)], axis=0)
        for i in range(few):
            mix_s[:, at[i]] = mix_s[:, at[i]] * keeps[i] + _dot(values, weights[i], 1, 0)

    for which in (0, 1):
        if which == 1:
            arrive_x(W1, 5)
            arrive_x(W1, 6)
            shared(3)
            shared(4)
            arrive(KV, 0)
            arrive(WO, 0, False)
        lax.fori_loop(which * few, (which + 1) * few, turn, None)
        block(me, 1, True, which * few)
        if which == 0:
            own_to_mate(KV, False).wait_recv()

        @pl.when(core == 1)
        def _():
            block(me - 1, 1, False, which * few)

    def step(t, _):
        def one(j, _):
            way, which = j // 2, j % 2

            for slot in sorted({slot for slot, _, _ in RELAYS}):
                @pl.when((t == slot[0]) & (j == slot[1]))
                def _():
                    for kind, n in (entry[1:] for entry in RELAYS if entry[0] == slot):
                        if kind == X:
                            arrive_x(WO, n)
                        elif n < 0:
                            begin(WO, (1,))
                        elif kind == ON:
                            forward(WO, n)
                        else:
                            arrive(kind, n, kind == KV)

            @pl.when((t < 4) & (j == 0))
            def _():
                from_mate(KV, t)

            @pl.when((t == 4) & (j == 0))
            def _():
                from_mate(KV, 4)

            of = _chip((place + (8 - t) * (1 - way) + t * way) % 8)

            @pl.when((of < chip) & ((way == 0) | (t < 4)))
            def _():
                block(of * 2, 2, False, which * few)

        lax.fori_loop(0, 4, one, None)

    lax.fori_loop(1, 5, step, None)

    def finish(h, _):
        at = pl.ds(pl.multiple_of(h * tokens, tokens), tokens)
        total = mix_s[head : head + 1, at]
        a_s[:, pl.ds(pl.multiple_of(head_of(h) * head, head), head)] = (mix_s[:head, at] * (1 / total)).T.astype(jnp.bfloat16)

    arrive(WO, 6)
    lax.fori_loop(0, heads, finish, None)

    def store(n):
        cols = pl.ds(pl.multiple_of(n * unit, unit), unit)
        return pltpu.make_async_copy(x_s.at[:, cols], out_hbm.at[:, cols], local.at[6 + n])

    def output(chips, fresh=False, last=False):
        rows = [pl.ds(pl.multiple_of(c * 2 * depth, 2 * depth), 2 * depth) for c in chips]

        def tile(n, _):
            cols = pl.ds(pl.multiple_of(n * unit, unit), unit)
            total = x_s[:, cols].astype(jnp.float32) if fresh else acc_s[:, cols]
            total += functools.reduce(jnp.add, [_dot(a_s[:, r], wo_s[r, cols], 1, 0) for r in rows])
            if last:
                x_s[:, cols] = total.astype(jnp.bfloat16)
                store(n).start()
            else:
                acc_s[:, cols] = total

        lax.fori_loop(0, dim // unit, tile, None)

    own_to_mate(WO, False).wait_recv()
    begun = sum(kind == X for _, kind, _ in RELAYS)
    t = 1
    for n in range(begun - 1, PIECES):
        if n >= begun:
            arrive_x(WO, n)
        while t < 4 and 2 * t - 1 <= n - (n >= begun):
            from_mate(WO, t)
            x_from_mate(WO, t)
            output([*([chip] if t == 1 else []), *(origin(way, t) for way in ways(t))], fresh=t == 1)
            t += 1
    from_mate(WO, 4)
    x_from_mate(WO, 4)
    output([origin(CW, 4)], last=True)

    for kind in (W1, KV, WO):
        own_to_mate(kind, True).wait_send()
        bulk(kind, 2 * PIECES, ring_cols(kind), ring_send.at[kind], d_recv.at[kind, 0]).wait_send()
        bulk(kind, 2 * PIECES, ring_cols(kind), d_send.at[kind], d_recv.at[kind, 0]).wait_send()
        if kind != KV:
            bulk(kind, 2 * x_pieces(kind), x_cols(kind, group), x_send.at[kind // 2], d_recv.at[kind, 0]).wait_send()
            bulk(kind, 2 * x_pieces(kind), x_cols(kind, 1 - group), dx_send.at[kind // 2], d_recv.at[kind, 0]).wait_send()
    for n in range(dim // unit):
        store(n).wait()


def attend(x, gain, wq, wk, wv, wo):
    half = wk.shape[1] // 2
    rate = THETA ** (-jnp.arange(half, dtype=jnp.float32) / half)
    (tokens, dim), depth, head = x.shape, wq.shape[0], wk.shape[1]
    heads = dim // head
    anywhere, vmem = pl.BlockSpec(memory_space=pl.ANY), pl.BlockSpec(memory_space=pltpu.VMEM)
    return pl.pallas_call(
        functools.partial(_kernel, shift={W1: 7 * dim // 16, WO: 7 * dim // 16}),
        out_shape=jax.ShapeDtypeStruct((tokens, dim), jnp.bfloat16),
        in_specs=[anywhere, vmem, vmem, anywhere, anywhere, anywhere, anywhere],
        out_specs=anywhere,
        scratch_shapes=[
            *[pltpu.VMEM((tokens, head // 2), jnp.float32)] * 2,
            pltpu.VMEM((tokens, dim), jnp.bfloat16),
            pltpu.VMEM((tokens, dim), jnp.bfloat16),
            pltpu.VMEM((16 * depth, dim + 2 * head), jnp.bfloat16),
            pltpu.VMEM((16 * depth, dim), jnp.bfloat16),
            pltpu.VMEM((16 * tokens, 2 * head), jnp.bfloat16),
            pltpu.VMEM((tokens, dim + 2 * head), jnp.float32),
            pltpu.VMEM((heads * tokens, head), jnp.bfloat16),
            pltpu.VMEM((1, heads * tokens), jnp.float32),
            pltpu.VMEM((head + 8, heads * tokens), jnp.float32),
            pltpu.SemaphoreType.DMA((10,)),
            *[pltpu.SemaphoreType.DMA(n) for n in ((3,), (3, 2, PIECES), (2,), (2, 2, PIECES), (3,), (3,), (3, 5), (2,), (2, 5))],
        ],
        compiler_params=pltpu.CompilerParams(collective_id=0, has_side_effects=True, vmem_limit_bytes=67043328),
    )(x, gain, rate[None], wq, wk, wv, wo)


def solution(mesh):
    tokens, whole = P(("dp", "sp"), None), P("sp", None)
    return jax.shard_map(
        attend,
        mesh=mesh,
        in_specs=(tokens, P(None), whole, whole, whole, whole),
        out_specs=tokens,
        check_vma=False,
    )
```

```python
import functools

import jax
import jax.numpy as jnp
from jax import lax
from jax.experimental import pallas as pl
from jax.experimental.pallas import tpu as pltpu
from jax.sharding import PartitionSpec as P

HEAD = 256
THETA = 10000
NEG = -1e30
HIDDEN = 2 * NEG
LOG2E = 1.4426950408889634
MESH = pl.DeviceIdType.MESH
CW, CCW = 0, 1
W1, KV, WO, X, ON = 0, 1, 2, 3, 4
PIECES = 7
RELAYS = (
    ((1, 0), KV, 1), ((1, 0), WO, -1), ((1, 2), KV, 2), ((1, 3), KV, 3), ((2, 0), ON, 2), ((2, 0), X, 0), ((2, 1), WO, 1), ((2, 1), ON, 3), ((2, 1), KV, 4),
    ((2, 3), KV, 5), ((3, 0), WO, 2), ((3, 0), ON, 4), ((3, 0), X, 1), ((3, 1), WO, 3), ((3, 1), ON, 5), ((3, 2), KV, 6), ((3, 3), X, 2), ((3, 3), WO, 4),
    ((3, 3), ON, 6), ((4, 0), WO, 5), ((4, 1), X, 3),
)


def _dot(a, b, ca, cb):
    return lax.dot_general(a, b, (((ca,), (cb,)), ((), ())), preferred_element_type=jnp.float32)


def _chip(p):
    y = p // 4
    return 4 * y + p + y * (7 - 2 * p)


def _lane(x, unit=128):
    return x if isinstance(x, int) else pl.multiple_of(x, unit)


def _kernel(x_hbm, gain_ref, rate_ref, wq_hbm, wk_hbm, wv_hbm, wo_hbm, out_ref,
            cos_s, sin_s, x_s, a_s, w1_s, wo_s, kv_s, acc_s, q_s, top_s, mix_s,
            local, ring_send, ring_recv, x_send, x_recv, own_send, d_send, d_recv, dx_send, dx_recv, *, shift):
    tokens, dim = x_s.shape
    depth = wq_hbm.shape[0]
    head = kv_s.shape[1] // 2
    heads = dim // head
    unit = 2 * head
    half = dim // 2
    group, me = lax.axis_index("dp"), lax.axis_index("sp")
    chip, core = me // 2, me % 2
    row = chip // 4
    z = chip % 4
    place = row * 7 + z - 2 * row * z

    def device(p):
        return (group, _chip(p % 8) * 2 + core)

    right, left, twin, mate = device(place + 1), device(place + 7), (1 - group, me), (group, chip * 2 + 1 - core)

    def origin(way, t):
        return _chip((place + 8 - t) % 8 if way == CW else (place + t) % 8)

    bufs = {W1: (w1_s, depth), KV: (kv_s, tokens), WO: (wo_s, depth)}

    def whole(kind):
        return (0, bufs[kind][0].shape[1])

    def window(kind, way, t, n, of_core, cols):
        buf, rows = bufs[kind]
        begin, width = cols
        part = rows // 2
        at = (origin(way, t) * 2 + of_core) * rows + (n % 2 if way == CW else 1 - n % 2) * part
        return buf.at[pl.ds(pl.multiple_of(at, part), part), pl.ds(_lane(begin), width)]

    def ring_cols(kind):
        full = whole(kind)[1]
        return (0, full) if kind == KV else (group * shift[kind], full - shift[kind])

    def x_cols(kind, of_group):
        return (of_group * (whole(kind)[1] - shift[kind]), shift[kind])

    def x_pieces(kind):
        return 0 if kind == KV else PIECES

    def copy(src, send, recv, to):
        return pltpu.make_async_remote_copy(src_ref=src, dst_ref=src, send_sem=send, recv_sem=recv, device_id=to, device_id_type=MESH)

    def ring(kind, way, n, sent):
        return copy(window(kind, way, n // 2 + (0 if sent else 1), n, core, ring_cols(kind)), ring_send.at[kind], ring_recv.at[kind, way, n],
                    right if way == CW else left)

    def over_x(kind, way, n, sent):
        return copy(window(kind, way, n // 2 + 1, n, core, x_cols(kind, group if sent else 1 - group)), x_send.at[kind // 2],
                    x_recv.at[kind // 2, way, n], twin)

    def to_mate(kind, way, n):
        return copy(window(kind, way, n // 2 + 1, n, core, ring_cols(kind)), d_send.at[kind], d_recv.at[kind, n // 2 + 1], mate)

    def x_to_mate(kind, way, n):
        return copy(window(kind, way, n // 2 + 1, n, core, x_cols(kind, 1 - group)), dx_send.at[kind // 2], dx_recv.at[kind // 2, n // 2 + 1], mate)

    def own_to_mate(kind, sent):
        buf, rows = bufs[kind]
        at = (chip * 2 + (core if sent else 1 - core)) * rows
        return copy(buf.at[pl.ds(pl.multiple_of(at, rows), rows), :], own_send.at[kind], d_recv.at[kind, 0], mate)

    def bulk(kind, count, cols, send, recv):
        buf, rows = bufs[kind]
        begin, width = cols
        return copy(buf.at[pl.ds(0, count * (rows // 2)), pl.ds(_lane(begin), width)], send, recv, mate)

    def begin(kind, pieces=(0, 1)):
        for n in pieces:
            ring(kind, CW, n, True).start()
            ring(kind, CCW, n, True).start()
        if pieces[0] == 0:
            own_to_mate(kind, True).start()

    def forward(kind, n):
        for way in (CW, CCW):
            ring(kind, way, n, True).start()

    def arrive(kind, n, onward=True):
        for way in (CW, CCW):
            ring(kind, way, n, False).wait_recv()
            if onward and n + 2 < PIECES:
                ring(kind, way, n + 2, True).start()
            if kind != KV:
                over_x(kind, way, n, True).start()
            to_mate(kind, way, n).start()

    def arrive_x(kind, n):
        for way in (CW, CCW):
            over_x(kind, way, n, False).wait_recv()
            x_to_mate(kind, way, n).start()

    def ways(t):
        return (CW, CCW) if t < 4 else (CW,)

    def from_mate(kind, t):
        count = 4 if not isinstance(t, int) or t < 4 else 2
        bulk(kind, count, ring_cols(kind), d_send.at[kind], d_recv.at[kind, t]).wait_recv()

    def x_from_mate(kind, t):
        bulk(kind, 4 if t < 4 else 2, x_cols(kind, 1 - group), dx_send.at[kind // 2], dx_recv.at[kind // 2, t]).wait_recv()

    own = pl.ds(pl.multiple_of(me * depth, depth), depth)
    loads = [
        (wq_hbm.at[:, pl.ds(0, half)], w1_s.at[own, pl.ds(0, half)]),
        (wk_hbm, w1_s.at[own, pl.ds(half, head)]),
        (wv_hbm, w1_s.at[own, pl.ds(half + head, head)]),
        (wq_hbm.at[:, pl.ds(half, half)], w1_s.at[own, pl.ds(half + unit, half)]),
        (x_hbm, x_s),
        (wo_hbm, wo_s.at[own, :]),
    ]
    loads = [pltpu.make_async_copy(src, dst, local.at[i]) for i, (src, dst) in enumerate(loads)]
    for load in loads:
        load.start()
    barrier = pltpu.get_barrier_semaphore()
    for to in (right, left, twin, mate):
        pl.semaphore_signal(barrier, inc=1, device_id=to, device_id_type=MESH)
    for load in loads[:4]:
        load.wait()
    pl.semaphore_wait(barrier, 4)
    begin(W1)

    loads[4].wait()
    gain = gain_ref[...].astype(jnp.float32)[None]
    some = min(64, tokens)

    def norm(i, _):
        here = pl.ds(pl.multiple_of(i * some, some), some)
        wide = x_s[here, :].astype(jnp.float32)
        scale = lax.rsqrt(jnp.mean(wide * wide, -1, keepdims=True) + 1e-6)
        a_s[here, :] = (wide * scale * gain).astype(jnp.bfloat16)

    lax.fori_loop(0, tokens // some, norm, None)
    spot = (me * tokens + lax.broadcasted_iota(jnp.int32, (tokens, head // 2), 0)).astype(jnp.float32)
    angle = spot * rate_ref[...]
    cos_s[...] = jnp.cos(angle)
    sin_s[...] = jnp.sin(angle)

    def project(chip_of, first, count, fresh=False):
        rows = pl.ds(pl.multiple_of(chip_of * 2 * depth, 2 * depth), 2 * depth)
        cols_a = pl.ds(pl.multiple_of(chip_of * 2 * depth, 2 * depth), 2 * depth)

        def tile(n, _):
            cols = pl.ds(pl.multiple_of((first + n) * unit, unit), unit)
            term = _dot(a_s[:, cols_a], w1_s[rows, cols], 1, 0)
            acc_s[:, cols] = term if fresh else acc_s[:, cols] + term

        lax.fori_loop(0, count, tile, None)

    mid = half // unit

    own_to_mate(W1, False).wait_recv()
    project(chip, 0, 2 * mid + 1, fresh=True)

    def shared(t):
        x_from_mate(W1, t)
        for way in ways(t):
            project(origin(way, t), (1 - group) * (mid + 1), mid)

    def carried(t):
        from_mate(W1, t)
        for way in ways(t):
            project(origin(way, t), group * mid, mid + 1)

    def keys_values(t):
        from_mate(W1, t)
        for way in ways(t):
            project(origin(way, t), mid, 1)

    def queries(t):
        for way in ways(t):
            project(origin(way, t), group * (mid + 1), mid)

    for n in range(PIECES):
        arrive(W1, n)
        if n == 5:
            loads[5].wait()
            begin(WO, (0,))
        if n in (2, 4):
            carried(n // 2)
        if n == 6:
            keys_values(3)
        if n == 4:
            shared(1)
        if 2 <= n < 6:
            arrive_x(W1, n - 2)
    keys_values(4)


    cos, sin = cos_s[...], sin_s[...]

    def turned(t):
        t = t.astype(jnp.bfloat16).astype(jnp.float32)
        a, b = t[:, : head // 2], t[:, head // 2 :]
        return jnp.concatenate([a * cos - b * sin, b * cos + a * sin], -1).astype(jnp.bfloat16)

    here = pl.multiple_of(me * tokens, tokens)
    kv_s[pl.ds(here, tokens), :head] = turned(acc_s[:, half : half + head])
    part = tokens // 2
    for j in range(2):
        value = acc_s[j * part : (j + 1) * part, half + head : half + unit].astype(jnp.bfloat16)
        kv_s[pl.ds(here + j * part, part), head:] = value.T if value.shape[0] == value.shape[1] else value
    begin(KV)
    arrive_x(W1, 4)
    queries(3)
    queries(4)
    shared(2)

    def head_of(i):
        return (i + group * (heads // 2)) % heads

    def turn(i, _):
        h = head_of(i)
        cols = pl.ds(pl.multiple_of(h * head + (h // (heads // 2)) * unit, head), head)
        q_s[pl.ds(pl.multiple_of(i * tokens, tokens), tokens), :] = turned(acc_s[:, cols])

    e = head**-0.5 * LOG2E
    top_s[...] = jnp.full(top_s.shape, NEG, jnp.float32)
    mix_s[...] = jnp.zeros(mix_s.shape, jnp.float32)

    few = heads // 2

    def block(first, count, masked, begin):
        base = pl.multiple_of(first * tokens, tokens)
        at = [pl.ds(pl.multiple_of((begin + i) * tokens, tokens), tokens) for i in range(few)]
        keys = kv_s[pl.ds(base, count * tokens), :head]
        scores = [_dot(keys, q_s[at[i], :], 1, 1) for i in range(few)]
        if masked:
            ok = lax.broadcasted_iota(jnp.int32, (tokens, tokens), 0) <= lax.broadcasted_iota(jnp.int32, (tokens, tokens), 1)
            scores = [jnp.where(ok, s, HIDDEN) for s in scores]
        weights, keeps = [], []
        for i, s in enumerate(scores):
            old = top_s[:, at[i]]
            top = jnp.maximum(old, s.max(axis=0, keepdims=True))
            top_s[:, at[i]] = top
            weights.append(jnp.exp2((s - top) * e).astype(jnp.bfloat16))
            keeps.append(jnp.exp2((old - top) * e))
        values = jnp.concatenate([kv_s[pl.ds(base + j * part, part), head:] for j in range(2 * count)], axis=1)
        values = jnp.concatenate([values, jnp.ones((8, count * tokens), jnp.bfloat16)], axis=0)
        for i in range(few):
            mix_s[:, at[i]] = mix_s[:, at[i]] * keeps[i] + _dot(values, weights[i], 1, 0)

    for which in (0, 1):
        if which == 1:
            arrive_x(W1, 5)
            arrive_x(W1, 6)
            shared(3)
            shared(4)
            arrive(KV, 0)
            arrive(WO, 0, False)
        lax.fori_loop(which * few, (which + 1) * few, turn, None)
        block(me, 1, True, which * few)
        if which == 0:
            own_to_mate(KV, False).wait_recv()

        @pl.when(core == 1)
        def _():
            block(me - 1, 1, False, which * few)

    def step(t, _):
        def one(j, _):
            way, which = j // 2, j % 2

            for slot in sorted({slot for slot, _, _ in RELAYS}):
                @pl.when((t == slot[0]) & (j == slot[1]))
                def _():
                    for kind, n in (entry[1:] for entry in RELAYS if entry[0] == slot):
                        if kind == X:
                            arrive_x(WO, n)
                        elif n < 0:
                            begin(WO, (1,))
                        elif kind == ON:
                            forward(WO, n)
                        else:
                            arrive(kind, n, kind == KV)

            @pl.when((t < 4) & (j == 0))
            def _():
                from_mate(KV, t)

            @pl.when((t == 4) & (j == 0))
            def _():
                from_mate(KV, 4)

            of = _chip((place + (8 - t) * (1 - way) + t * way) % 8)

            @pl.when((of < chip) & ((way == 0) | (t < 4)))
            def _():
                block(of * 2, 2, False, which * few)

        lax.fori_loop(0, 4, one, None)

    lax.fori_loop(1, 5, step, None)

    def finish(h, _):
        at = pl.ds(pl.multiple_of(h * tokens, tokens), tokens)
        total = mix_s[head : head + 1, at]
        a_s[:, pl.ds(pl.multiple_of(head_of(h) * head, head), head)] = (mix_s[:head, at] * (1 / total)).T.astype(jnp.bfloat16)

    arrive(WO, 6)
    lax.fori_loop(0, heads, finish, None)

    def output(chips, fresh=False, last=False):
        rows = [pl.ds(pl.multiple_of(c * 2 * depth, 2 * depth), 2 * depth) for c in chips]

        def tile(n, _):
            cols = pl.ds(pl.multiple_of(n * unit, unit), unit)
            total = x_s[:, cols].astype(jnp.float32) if fresh else acc_s[:, cols]
            total += functools.reduce(jnp.add, [_dot(a_s[:, r], wo_s[r, cols], 1, 0) for r in rows])
            if last:
                out_ref[:, cols] = total.astype(jnp.bfloat16)
            else:
                acc_s[:, cols] = total

        lax.fori_loop(0, dim // unit, tile, None)

    own_to_mate(WO, False).wait_recv()
    begun = sum(kind == X for _, kind, _ in RELAYS)
    t = 1
    for n in range(begun - 1, PIECES):
        if n >= begun:
            arrive_x(WO, n)
        while t < 4 and 2 * t - 1 <= n - (n >= begun):
            from_mate(WO, t)
            x_from_mate(WO, t)
            output([*([chip] if t == 1 else []), *(origin(way, t) for way in ways(t))], fresh=t == 1)
            t += 1
    from_mate(WO, 4)
    x_from_mate(WO, 4)
    output([origin(CW, 4)], last=True)

    for kind in (W1, KV, WO):
        own_to_mate(kind, True).wait_send()
        bulk(kind, 2 * PIECES, ring_cols(kind), ring_send.at[kind], d_recv.at[kind, 0]).wait_send()
        bulk(kind, 2 * PIECES, ring_cols(kind), d_send.at[kind], d_recv.at[kind, 0]).wait_send()
        if kind != KV:
            bulk(kind, 2 * x_pieces(kind), x_cols(kind, group), x_send.at[kind // 2], d_recv.at[kind, 0]).wait_send()
            bulk(kind, 2 * x_pieces(kind), x_cols(kind, 1 - group), dx_send.at[kind // 2], d_recv.at[kind, 0]).wait_send()


def attend(x, gain, wq, wk, wv, wo):
    half = wk.shape[1] // 2
    rate = THETA ** (-jnp.arange(half, dtype=jnp.float32) / half)
    (tokens, dim), depth, head = x.shape, wq.shape[0], wk.shape[1]
    heads = dim // head
    anywhere, vmem = pl.BlockSpec(memory_space=pl.ANY), pl.BlockSpec(memory_space=pltpu.VMEM)
    return pl.pallas_call(
        functools.partial(_kernel, shift={W1: 7 * dim // 16, WO: 7 * dim // 16}),
        out_shape=pltpu.VMEM((tokens, dim), jnp.bfloat16),
        in_specs=[anywhere, vmem, vmem, anywhere, anywhere, anywhere, anywhere],
        out_specs=vmem,
        scratch_shapes=[
            *[pltpu.VMEM((tokens, head // 2), jnp.float32)] * 2,
            pltpu.VMEM((tokens, dim), jnp.bfloat16),
            pltpu.VMEM((tokens, dim), jnp.bfloat16),
            pltpu.VMEM((16 * depth, dim + 2 * head), jnp.bfloat16),
            pltpu.VMEM((16 * depth, dim), jnp.bfloat16),
            pltpu.VMEM((16 * tokens, 2 * head), jnp.bfloat16),
            pltpu.VMEM((tokens, dim + 2 * head), jnp.float32),
            pltpu.VMEM((heads * tokens, head), jnp.bfloat16),
            pltpu.VMEM((1, heads * tokens), jnp.float32),
            pltpu.VMEM((head + 8, heads * tokens), jnp.float32),
            pltpu.SemaphoreType.DMA((6,)),
            *[pltpu.SemaphoreType.DMA(n) for n in ((3,), (3, 2, PIECES), (2,), (2, 2, PIECES), (3,), (3,), (3, 5), (2,), (2, 5))],
        ],
        compiler_params=pltpu.CompilerParams(collective_id=0, has_side_effects=True, vmem_limit_bytes=60 * 2**20),
    )(x, gain, rate[None], wq, wk, wv, wo)


def solution(mesh):
    tokens, whole = P(("dp", "sp"), None), P("sp", None)
    return jax.shard_map(
        attend,
        mesh=mesh,
        in_specs=(tokens, P(None), whole, whole, whole, whole),
        out_specs=tokens,
        check_vma=False,
    )
```

```python
import functools

import jax
import jax.numpy as jnp
from jax import lax
from jax.experimental import pallas as pl
from jax.experimental.pallas import tpu as pltpu
from jax.sharding import PartitionSpec as P

HEAD = 256
THETA = 10000
NEG = -1e30
HIDDEN = 2 * NEG
LOG2E = 1.4426950408889634
MESH = pl.DeviceIdType.MESH
CW, CCW = 0, 1
W1, KV, WO, X, ON = 0, 1, 2, 3, 4
PIECES = 7
RELAYS = (
    ((1, 0), KV, 1), ((1, 0), WO, -1), ((1, 2), KV, 2), ((2, 0), KV, 3), ((2, 0), ON, 2), ((2, 0), X, 0), ((2, 1), WO, 1), ((2, 1), ON, 3), ((2, 1), KV, 4),
    ((2, 3), KV, 5), ((3, 0), WO, 2), ((3, 0), ON, 4), ((3, 0), X, 1), ((3, 1), WO, 3), ((3, 1), ON, 5), ((3, 2), KV, 6), ((3, 3), X, 2), ((3, 3), WO, 4),
    ((3, 3), ON, 6), ((4, 0), WO, 5), ((4, 1), X, 3),
)


def _dot(a, b, ca, cb):
    return lax.dot_general(a, b, (((ca,), (cb,)), ((), ())), preferred_element_type=jnp.float32)


def _chip(p):
    y = p // 4
    return 4 * y + p + y * (7 - 2 * p)


def _lane(x, unit=128):
    return x if isinstance(x, int) else pl.multiple_of(x, unit)


def _kernel(x_hbm, gain_ref, rate_ref, wq_hbm, wk_hbm, wv_hbm, wo_hbm, out_ref,
            cos_s, sin_s, x_s, a_s, w1_s, wo_s, kv_s, acc_s, q_s, top_s, mix_s,
            local, ring_send, ring_recv, x_send, x_recv, own_send, d_send, d_recv, dx_send, dx_recv, *, shift):
    tokens, dim = x_s.shape
    depth = wq_hbm.shape[0]
    head = kv_s.shape[1] // 2
    heads = dim // head
    unit = 2 * head
    half = dim // 2
    group, me = lax.axis_index("dp"), lax.axis_index("sp")
    chip, core = me // 2, me % 2
    row = chip // 4
    z = chip % 4
    place = row * 7 + z - 2 * row * z

    def device(p):
        return (group, _chip(p % 8) * 2 + core)

    right, left, twin, mate = device(place + 1), device(place + 7), (1 - group, me), (group, chip * 2 + 1 - core)

    def origin(way, t):
        return _chip((place + 8 - t) % 8 if way == CW else (place + t) % 8)

    bufs = {W1: (w1_s, depth), KV: (kv_s, tokens), WO: (wo_s, depth)}

    def whole(kind):
        return (0, bufs[kind][0].shape[1])

    def window(kind, way, t, n, of_core, cols):
        buf, rows = bufs[kind]
        begin, width = cols
        part = rows // 2
        at = (origin(way, t) * 2 + of_core) * rows + (n % 2 if way == CW else 1 - n % 2) * part
        return buf.at[pl.ds(pl.multiple_of(at, part), part), pl.ds(_lane(begin), width)]

    def ring_cols(kind):
        full = whole(kind)[1]
        return (0, full) if kind == KV else (group * shift[kind], full - shift[kind])

    def x_cols(kind, of_group):
        return (of_group * (whole(kind)[1] - shift[kind]), shift[kind])

    def x_pieces(kind):
        return 0 if kind == KV else PIECES

    def copy(src, send, recv, to):
        return pltpu.make_async_remote_copy(src_ref=src, dst_ref=src, send_sem=send, recv_sem=recv, device_id=to, device_id_type=MESH)

    def ring(kind, way, n, sent):
        return copy(window(kind, way, n // 2 + (0 if sent else 1), n, core, ring_cols(kind)), ring_send.at[kind], ring_recv.at[kind, way, n],
                    right if way == CW else left)

    def over_x(kind, way, n, sent):
        return copy(window(kind, way, n // 2 + 1, n, core, x_cols(kind, group if sent else 1 - group)), x_send.at[kind // 2],
                    x_recv.at[kind // 2, way, n], twin)

    def to_mate(kind, way, n):
        return copy(window(kind, way, n // 2 + 1, n, core, ring_cols(kind)), d_send.at[kind], d_recv.at[kind, n // 2 + 1], mate)

    def x_to_mate(kind, way, n):
        return copy(window(kind, way, n // 2 + 1, n, core, x_cols(kind, 1 - group)), dx_send.at[kind // 2], dx_recv.at[kind // 2, n // 2 + 1], mate)

    def own_to_mate(kind, sent):
        buf, rows = bufs[kind]
        at = (chip * 2 + (core if sent else 1 - core)) * rows
        return copy(buf.at[pl.ds(pl.multiple_of(at, rows), rows), :], own_send.at[kind], d_recv.at[kind, 0], mate)

    def bulk(kind, count, cols, send, recv):
        buf, rows = bufs[kind]
        begin, width = cols
        return copy(buf.at[pl.ds(0, count * (rows // 2)), pl.ds(_lane(begin), width)], send, recv, mate)

    def begin(kind, pieces=(0, 1)):
        for n in pieces:
            ring(kind, CW, n, True).start()
            ring(kind, CCW, n, True).start()
        if pieces[0] == 0:
            own_to_mate(kind, True).start()

    def forward(kind, n):
        for way in (CW, CCW):
            ring(kind, way, n, True).start()

    def arrive(kind, n, onward=True):
        for way in (CW, CCW):
            ring(kind, way, n, False).wait_recv()
            if onward and n + 2 < PIECES:
                ring(kind, way, n + 2, True).start()
            if kind != KV:
                over_x(kind, way, n, True).start()
            to_mate(kind, way, n).start()

    def arrive_x(kind, n):
        for way in (CW, CCW):
            over_x(kind, way, n, False).wait_recv()
            x_to_mate(kind, way, n).start()

    def ways(t):
        return (CW, CCW) if t < 4 else (CW,)

    def from_mate(kind, t):
        count = 4 if not isinstance(t, int) or t < 4 else 2
        bulk(kind, count, ring_cols(kind), d_send.at[kind], d_recv.at[kind, t]).wait_recv()

    def x_from_mate(kind, t):
        bulk(kind, 4 if t < 4 else 2, x_cols(kind, 1 - group), dx_send.at[kind // 2], dx_recv.at[kind // 2, t]).wait_recv()

    own = pl.ds(pl.multiple_of(me * depth, depth), depth)
    loads = [
        (wq_hbm.at[:, pl.ds(0, half)], w1_s.at[own, pl.ds(0, half)]),
        (wk_hbm, w1_s.at[own, pl.ds(half, head)]),
        (wv_hbm, w1_s.at[own, pl.ds(half + head, head)]),
        (wq_hbm.at[:, pl.ds(half, half)], w1_s.at[own, pl.ds(half + unit, half)]),
        (x_hbm, x_s),
        (wo_hbm, wo_s.at[own, :]),
    ]
    loads = [pltpu.make_async_copy(src, dst, local.at[i]) for i, (src, dst) in enumerate(loads)]
    for load in loads:
        load.start()
    barrier = pltpu.get_barrier_semaphore()
    for to in (right, left, twin, mate):
        pl.semaphore_signal(barrier, inc=1, device_id=to, device_id_type=MESH)
    for load in loads[:4]:
        load.wait()
    pl.semaphore_wait(barrier, 4)
    begin(W1)

    loads[4].wait()
    gain = gain_ref[...].astype(jnp.float32)[None]
    some = min(64, tokens)

    def norm(i, _):
        here = pl.ds(pl.multiple_of(i * some, some), some)
        wide = x_s[here, :].astype(jnp.float32)
        scale = lax.rsqrt(jnp.mean(wide * wide, -1, keepdims=True) + 1e-6)
        a_s[here, :] = (wide * scale * gain).astype(jnp.bfloat16)

    lax.fori_loop(0, tokens // some, norm, None)
    spot = (me * tokens + lax.broadcasted_iota(jnp.int32, (tokens, head // 2), 0)).astype(jnp.float32)
    angle = spot * rate_ref[...]
    cos_s[...] = jnp.cos(angle)
    sin_s[...] = jnp.sin(angle)

    def project(chip_of, first, count, fresh=False):
        rows = pl.ds(pl.multiple_of(chip_of * 2 * depth, 2 * depth), 2 * depth)
        cols_a = pl.ds(pl.multiple_of(chip_of * 2 * depth, 2 * depth), 2 * depth)

        def tile(n, _):
            cols = pl.ds(pl.multiple_of((first + n) * unit, unit), unit)
            term = _dot(a_s[:, cols_a], w1_s[rows, cols], 1, 0)
            acc_s[:, cols] = term if fresh else acc_s[:, cols] + term

        lax.fori_loop(0, count, tile, None)

    mid = half // unit

    own_to_mate(W1, False).wait_recv()
    project(chip, 0, 2 * mid + 1, fresh=True)

    def shared(t):
        x_from_mate(W1, t)
        for way in ways(t):
            project(origin(way, t), (1 - group) * (mid + 1), mid)

    def carried(t):
        from_mate(W1, t)
        for way in ways(t):
            project(origin(way, t), group * mid, mid + 1)

    def keys_values(t):
        from_mate(W1, t)
        for way in ways(t):
            project(origin(way, t), mid, 1)

    def queries(t):
        for way in ways(t):
            project(origin(way, t), group * (mid + 1), mid)

    for n in range(PIECES):
        arrive(W1, n)
        if n == 5:
            loads[5].wait()
            begin(WO, (0,))
        if n in (2, 4):
            carried(n // 2)
        if n == 6:
            keys_values(3)
        if n == 4:
            shared(1)
        if 2 <= n < 6:
            arrive_x(W1, n - 2)
    keys_values(4)


    cos, sin = cos_s[...], sin_s[...]

    def turned(t):
        t = t.astype(jnp.bfloat16).astype(jnp.float32)
        a, b = t[:, : head // 2], t[:, head // 2 :]
        return jnp.concatenate([a * cos - b * sin, b * cos + a * sin], -1).astype(jnp.bfloat16)

    here = pl.multiple_of(me * tokens, tokens)
    kv_s[pl.ds(here, tokens), :head] = turned(acc_s[:, half : half + head])
    part = tokens // 2
    for j in range(2):
        value = acc_s[j * part : (j + 1) * part, half + head : half + unit].astype(jnp.bfloat16)
        kv_s[pl.ds(here + j * part, part), head:] = value.T if value.shape[0] == value.shape[1] else value
    begin(KV)
    arrive_x(W1, 4)
    queries(3)
    queries(4)
    shared(2)

    def head_of(i):
        return (i + group * (heads // 2)) % heads

    def turn(i, _):
        h = head_of(i)
        cols = pl.ds(pl.multiple_of(h * head + (h // (heads // 2)) * unit, head), head)
        q_s[pl.ds(pl.multiple_of(i * tokens, tokens), tokens), :] = turned(acc_s[:, cols])

    e = head**-0.5 * LOG2E
    top_s[...] = jnp.full(top_s.shape, NEG, jnp.float32)
    mix_s[...] = jnp.zeros(mix_s.shape, jnp.float32)

    few = heads // 2

    def block(first, count, masked, begin):
        base = pl.multiple_of(first * tokens, tokens)
        at = [pl.ds(pl.multiple_of((begin + i) * tokens, tokens), tokens) for i in range(few)]
        keys = kv_s[pl.ds(base, count * tokens), :head]
        if masked:
            ok = lax.broadcasted_iota(jnp.int32, (tokens, tokens), 0) <= lax.broadcasted_iota(jnp.int32, (tokens, tokens), 1)
        values = jnp.concatenate([kv_s[pl.ds(base + j * part, part), head:] for j in range(2 * count)], axis=1)
        values = jnp.concatenate([values, jnp.ones((8, count * tokens), jnp.bfloat16)], axis=0)

        def score(i):
            s = _dot(keys, q_s[at[i], :], 1, 1)
            return jnp.where(ok, s, HIDDEN) if masked else s

        def soft(i, s):
            old = top_s[:, at[i]]
            top = jnp.maximum(old, s.max(axis=0, keepdims=True))
            top_s[:, at[i]] = top
            return jnp.exp2((s - top) * e).astype(jnp.bfloat16), jnp.exp2((old - top) * e)

        def mix(i, weight, keep):
            mix_s[:, at[i]] = mix_s[:, at[i]] * keep + _dot(values, weight, 1, 0)

        s0 = score(0)
        s1 = score(1)
        w0 = soft(0, s0)
        s2 = score(2)
        w1 = soft(1, s1)
        mix(0, *w0)
        s3 = score(3)
        w2 = soft(2, s2)
        mix(1, *w1)
        w3 = soft(3, s3)
        mix(2, *w2)
        mix(3, *w3)

    for which in (0, 1):
        if which == 1:
            arrive_x(W1, 5)
            arrive_x(W1, 6)
            shared(3)
            shared(4)
            arrive(KV, 0)
            arrive(WO, 0, False)
        lax.fori_loop(which * few, (which + 1) * few, turn, None)
        block(me, 1, True, which * few)
        if which == 0:
            own_to_mate(KV, False).wait_recv()

        @pl.when(core == 1)
        def _():
            block(me - 1, 1, False, which * few)

    def step(t, _):
        def one(j, _):
            way, which = j // 2, j % 2

            for slot in sorted({slot for slot, _, _ in RELAYS}):
                @pl.when((t == slot[0]) & (j == slot[1]))
                def _():
                    for kind, n in (entry[1:] for entry in RELAYS if entry[0] == slot):
                        if kind == X:
                            arrive_x(WO, n)
                        elif n < 0:
                            begin(WO, (1,))
                        elif kind == ON:
                            forward(WO, n)
                        else:
                            arrive(kind, n, kind == KV)

            @pl.when((t < 4) & (j == 0))
            def _():
                from_mate(KV, t)

            @pl.when((t == 4) & (j == 0))
            def _():
                from_mate(KV, 4)

            of = _chip((place + (8 - t) * (1 - way) + t * way) % 8)

            @pl.when((of < chip) & ((way == 0) | (t < 4)))
            def _():
                block(of * 2, 2, False, which * few)

        lax.fori_loop(0, 4, one, None)

    lax.fori_loop(1, 5, step, None)

    def finish(h, _):
        at = pl.ds(pl.multiple_of(h * tokens, tokens), tokens)
        total = mix_s[head : head + 1, at]
        a_s[:, pl.ds(pl.multiple_of(head_of(h) * head, head), head)] = (mix_s[:head, at] * (1 / total)).T.astype(jnp.bfloat16)

    arrive(WO, 6)
    lax.fori_loop(0, heads, finish, None)

    def output(chips, fresh=False, last=False):
        rows = [pl.ds(pl.multiple_of(c * 2 * depth, 2 * depth), 2 * depth) for c in chips]

        def tile(n, _):
            cols = pl.ds(pl.multiple_of(n * unit, unit), unit)
            total = x_s[:, cols].astype(jnp.float32) if fresh else acc_s[:, cols]
            total += functools.reduce(jnp.add, [_dot(a_s[:, r], wo_s[r, cols], 1, 0) for r in rows])
            if last:
                out_ref[:, cols] = total.astype(jnp.bfloat16)
            else:
                acc_s[:, cols] = total

        lax.fori_loop(0, dim // unit, tile, None)

    own_to_mate(WO, False).wait_recv()
    begun = sum(kind == X for _, kind, _ in RELAYS)
    t = 1
    for n in range(begun - 1, PIECES):
        if n >= begun:
            arrive_x(WO, n)
        while t < 4 and 2 * t - 1 <= n - (n >= begun):
            from_mate(WO, t)
            x_from_mate(WO, t)
            output([*([chip] if t == 1 else []), *(origin(way, t) for way in ways(t))], fresh=t == 1)
            t += 1
    from_mate(WO, 4)
    x_from_mate(WO, 4)
    output([origin(CW, 4)], last=True)

    for kind in (W1, KV, WO):
        own_to_mate(kind, True).wait_send()
        bulk(kind, 2 * PIECES, ring_cols(kind), ring_send.at[kind], d_recv.at[kind, 0]).wait_send()
        bulk(kind, 2 * PIECES, ring_cols(kind), d_send.at[kind], d_recv.at[kind, 0]).wait_send()
        if kind != KV:
            bulk(kind, 2 * x_pieces(kind), x_cols(kind, group), x_send.at[kind // 2], d_recv.at[kind, 0]).wait_send()
            bulk(kind, 2 * x_pieces(kind), x_cols(kind, 1 - group), dx_send.at[kind // 2], d_recv.at[kind, 0]).wait_send()


def attend(x, gain, wq, wk, wv, wo):
    half = wk.shape[1] // 2
    rate = THETA ** (-jnp.arange(half, dtype=jnp.float32) / half)
    (tokens, dim), depth, head = x.shape, wq.shape[0], wk.shape[1]
    heads = dim // head
    anywhere, vmem = pl.BlockSpec(memory_space=pl.ANY), pl.BlockSpec(memory_space=pltpu.VMEM)
    return pl.pallas_call(
        functools.partial(_kernel, shift={W1: 7 * dim // 16, WO: 7 * dim // 16}),
        out_shape=pltpu.VMEM((tokens, dim), jnp.bfloat16),
        in_specs=[anywhere, vmem, vmem, anywhere, anywhere, anywhere, anywhere],
        out_specs=vmem,
        scratch_shapes=[
            *[pltpu.VMEM((tokens, head // 2), jnp.float32)] * 2,
            pltpu.VMEM((tokens, dim), jnp.bfloat16),
            pltpu.VMEM((tokens, dim), jnp.bfloat16),
            pltpu.VMEM((16 * depth, dim + 2 * head), jnp.bfloat16),
            pltpu.VMEM((16 * depth, dim), jnp.bfloat16),
            pltpu.VMEM((16 * tokens, 2 * head), jnp.bfloat16),
            pltpu.VMEM((tokens, dim + 2 * head), jnp.float32),
            pltpu.VMEM((heads * tokens, head), jnp.bfloat16),
            pltpu.VMEM((1, heads * tokens), jnp.float32),
            pltpu.VMEM((head + 8, heads * tokens), jnp.float32),
            pltpu.SemaphoreType.DMA((6,)),
            *[pltpu.SemaphoreType.DMA(n) for n in ((3,), (3, 2, PIECES), (2,), (2, 2, PIECES), (3,), (3,), (3, 5), (2,), (2, 5))],
        ],
        compiler_params=pltpu.CompilerParams(collective_id=0, has_side_effects=True, vmem_limit_bytes=60 * 2**20),
    )(x, gain, rate[None], wq, wk, wv, wo)


def solution(mesh):
    tokens, whole = P(("dp", "sp"), None), P("sp", None)
    return jax.shard_map(
        attend,
        mesh=mesh,
        in_specs=(tokens, P(None), whole, whole, whole, whole),
        out_specs=tokens,
        check_vma=False,
    )
```

```python
import functools

import jax
import jax.numpy as jnp
from jax import lax
from jax.experimental import pallas as pl
from jax.experimental.pallas import tpu as pltpu
from jax.sharding import PartitionSpec as P

HEAD = 256
THETA = 10000
NEG = -1e30
HIDDEN = 2 * NEG
LOG2E = 1.4426950408889634
MESH = pl.DeviceIdType.MESH
CW, CCW = 0, 1
W1, KV, WO, X, ON = 0, 1, 2, 3, 4
PIECES = 7
RELAYS = (
    ((1, 0), KV, 1), ((1, 0), WO, -1), ((1, 2), KV, 2), ((2, 0), KV, 3), ((2, 0), ON, 2), ((2, 0), X, 0), ((2, 1), WO, 1), ((2, 1), ON, 3), ((2, 1), KV, 4),
    ((2, 3), KV, 5), ((3, 0), WO, 2), ((3, 0), ON, 4), ((3, 0), X, 1), ((3, 1), WO, 3), ((3, 1), ON, 5), ((3, 2), KV, 6), ((3, 3), X, 2), ((3, 3), WO, 4),
    ((3, 3), ON, 6), ((4, 0), WO, 5), ((4, 1), X, 3),
)


def _dot(a, b, ca, cb):
    return lax.dot_general(a, b, (((ca,), (cb,)), ((), ())), preferred_element_type=jnp.float32)


def _chip(p):
    y = p // 4
    return 4 * y + p + y * (7 - 2 * p)


def _lane(x, unit=128):
    return x if isinstance(x, int) else pl.multiple_of(x, unit)


def _kernel(x_hbm, gain_ref, rate_ref, wq_hbm, wk_hbm, wv_hbm, wo_hbm, out_ref,
            cos_s, sin_s, x_s, a_s, w1_s, wo_s, kv_s, acc_s, q_s, top_s, mix_s,
            local, ring_send, ring_recv, x_send, x_recv, own_send, d_send, d_recv, dx_send, dx_recv, *, shift):
    tokens, dim = x_s.shape
    depth = wq_hbm.shape[0]
    head = kv_s.shape[1] // 2
    heads = dim // head
    unit = 2 * head
    half = dim // 2
    group, me = lax.axis_index("dp"), lax.axis_index("sp")
    chip, core = me // 2, me % 2
    row = chip // 4
    z = chip % 4
    place = row * 7 + z - 2 * row * z

    def device(p):
        return (group, _chip(p % 8) * 2 + core)

    right, left, twin, mate = device(place + 1), device(place + 7), (1 - group, me), (group, chip * 2 + 1 - core)

    def origin(way, t):
        return _chip((place + 8 - t) % 8 if way == CW else (place + t) % 8)

    bufs = {W1: (w1_s, depth), KV: (kv_s, tokens), WO: (wo_s, depth)}

    def whole(kind):
        return (0, bufs[kind][0].shape[1])

    def window(kind, way, t, n, of_core, cols):
        buf, rows = bufs[kind]
        begin, width = cols
        part = rows // 2
        at = (origin(way, t) * 2 + of_core) * rows + (n % 2 if way == CW else 1 - n % 2) * part
        return buf.at[pl.ds(pl.multiple_of(at, part), part), pl.ds(_lane(begin), width)]

    def ring_cols(kind):
        full = whole(kind)[1]
        return (0, full) if kind == KV else (group * shift[kind], full - shift[kind])

    def x_cols(kind, of_group):
        return (of_group * (whole(kind)[1] - shift[kind]), shift[kind])

    def x_pieces(kind):
        return 0 if kind == KV else PIECES

    def copy(src, send, recv, to):
        return pltpu.make_async_remote_copy(src_ref=src, dst_ref=src, send_sem=send, recv_sem=recv, device_id=to, device_id_type=MESH)

    def ring(kind, way, n, sent):
        return copy(window(kind, way, n // 2 + (0 if sent else 1), n, core, ring_cols(kind)), ring_send.at[kind], ring_recv.at[kind, way, n],
                    right if way == CW else left)

    def over_x(kind, way, n, sent):
        return copy(window(kind, way, n // 2 + 1, n, core, x_cols(kind, group if sent else 1 - group)), x_send.at[kind // 2],
                    x_recv.at[kind // 2, way, n], twin)

    def to_mate(kind, way, n):
        return copy(window(kind, way, n // 2 + 1, n, core, ring_cols(kind)), d_send.at[kind], d_recv.at[kind, n // 2 + 1], mate)

    def x_to_mate(kind, way, n):
        return copy(window(kind, way, n // 2 + 1, n, core, x_cols(kind, 1 - group)), dx_send.at[kind // 2], dx_recv.at[kind // 2, n // 2 + 1], mate)

    def own_to_mate(kind, sent):
        buf, rows = bufs[kind]
        at = (chip * 2 + (core if sent else 1 - core)) * rows
        return copy(buf.at[pl.ds(pl.multiple_of(at, rows), rows), :], own_send.at[kind], d_recv.at[kind, 0], mate)

    def bulk(kind, count, cols, send, recv):
        buf, rows = bufs[kind]
        begin, width = cols
        return copy(buf.at[pl.ds(0, count * (rows // 2)), pl.ds(_lane(begin), width)], send, recv, mate)

    def begin(kind, pieces=(0, 1)):
        for n in pieces:
            ring(kind, CW, n, True).start()
            ring(kind, CCW, n, True).start()
        if pieces[0] == 0:
            own_to_mate(kind, True).start()

    def forward(kind, n):
        for way in (CW, CCW):
            ring(kind, way, n, True).start()

    def arrive(kind, n, onward=True):
        for way in (CW, CCW):
            ring(kind, way, n, False).wait_recv()
            if onward and n + 2 < PIECES:
                ring(kind, way, n + 2, True).start()
            if kind != KV:
                over_x(kind, way, n, True).start()
            to_mate(kind, way, n).start()

    def arrive_x(kind, n):
        for way in (CW, CCW):
            over_x(kind, way, n, False).wait_recv()
            x_to_mate(kind, way, n).start()

    def ways(t):
        return (CW, CCW) if t < 4 else (CW,)

    def from_mate(kind, t):
        count = 4 if not isinstance(t, int) or t < 4 else 2
        bulk(kind, count, ring_cols(kind), d_send.at[kind], d_recv.at[kind, t]).wait_recv()

    def x_from_mate(kind, t):
        bulk(kind, 4 if t < 4 else 2, x_cols(kind, 1 - group), dx_send.at[kind // 2], dx_recv.at[kind // 2, t]).wait_recv()

    own = pl.ds(pl.multiple_of(me * depth, depth), depth)
    loads = [
        (wq_hbm.at[:, pl.ds(0, half)], w1_s.at[own, pl.ds(0, half)]),
        (wk_hbm, w1_s.at[own, pl.ds(half, head)]),
        (wv_hbm, w1_s.at[own, pl.ds(half + head, head)]),
        (wq_hbm.at[:, pl.ds(half, half)], w1_s.at[own, pl.ds(half + unit, half)]),
        (x_hbm, x_s),
        (wo_hbm, wo_s.at[own, :]),
    ]
    loads = [pltpu.make_async_copy(src, dst, local.at[i]) for i, (src, dst) in enumerate(loads)]
    for load in loads:
        load.start()
    barrier = pltpu.get_barrier_semaphore()
    for to in (right, left, twin, mate):
        pl.semaphore_signal(barrier, inc=1, device_id=to, device_id_type=MESH)
    for load in loads[:4]:
        load.wait()
    pl.semaphore_wait(barrier, 4)
    begin(W1)

    loads[4].wait()
    gain = gain_ref[...].astype(jnp.float32)[None]
    some = min(64, tokens)

    def norm(i, _):
        here = pl.ds(pl.multiple_of(i * some, some), some)
        wide = x_s[here, :].astype(jnp.float32)
        scale = lax.rsqrt(jnp.mean(wide * wide, -1, keepdims=True) + 1e-6)
        a_s[here, :] = (wide * scale * gain).astype(jnp.bfloat16)

    lax.fori_loop(0, tokens // some, norm, None)
    spot = (me * tokens + lax.broadcasted_iota(jnp.int32, (tokens, head // 2), 0)).astype(jnp.float32)
    angle = spot * rate_ref[...]
    cos_s[...] = jnp.cos(angle)
    sin_s[...] = jnp.sin(angle)

    def project(chip_of, first, count, fresh=False):
        rows = pl.ds(pl.multiple_of(chip_of * 2 * depth, 2 * depth), 2 * depth)
        cols_a = pl.ds(pl.multiple_of(chip_of * 2 * depth, 2 * depth), 2 * depth)

        def tile(n, _):
            cols = pl.ds(pl.multiple_of((first + n) * unit, unit), unit)
            term = _dot(a_s[:, cols_a], w1_s[rows, cols], 1, 0)
            acc_s[:, cols] = term if fresh else acc_s[:, cols] + term

        lax.fori_loop(0, count, tile, None)

    mid = half // unit

    own_to_mate(W1, False).wait_recv()
    project(chip, 0, 2 * mid + 1, fresh=True)

    def shared(t):
        x_from_mate(W1, t)
        for way in ways(t):
            project(origin(way, t), (1 - group) * (mid + 1), mid)

    def carried(t):
        from_mate(W1, t)
        for way in ways(t):
            project(origin(way, t), group * mid, mid + 1)

    def keys_values(t):
        from_mate(W1, t)
        for way in ways(t):
            project(origin(way, t), mid, 1)

    def queries(t):
        for way in ways(t):
            project(origin(way, t), group * (mid + 1), mid)

    for n in range(PIECES):
        arrive(W1, n)
        if n == 6:
            loads[5].wait()
            begin(WO, (0,))
        if n in (2, 4):
            carried(n // 2)
        if n == 6:
            keys_values(3)
        if n == 4:
            shared(1)
        if 2 <= n < 6:
            arrive_x(W1, n - 2)
    keys_values(4)


    cos, sin = cos_s[...], sin_s[...]

    def turned(t):
        t = t.astype(jnp.bfloat16).astype(jnp.float32)
        a, b = t[:, : head // 2], t[:, head // 2 :]
        return jnp.concatenate([a * cos - b * sin, b * cos + a * sin], -1).astype(jnp.bfloat16)

    here = pl.multiple_of(me * tokens, tokens)
    kv_s[pl.ds(here, tokens), :head] = turned(acc_s[:, half : half + head])
    part = tokens // 2
    for j in range(2):
        value = acc_s[j * part : (j + 1) * part, half + head : half + unit].astype(jnp.bfloat16)
        kv_s[pl.ds(here + j * part, part), head:] = value.T if value.shape[0] == value.shape[1] else value
    begin(KV)
    arrive_x(W1, 4)
    queries(3)
    queries(4)
    shared(2)

    def head_of(i):
        return (i + group * (heads // 2)) % heads

    def turn(i, _):
        h = head_of(i)
        cols = pl.ds(pl.multiple_of(h * head + (h // (heads // 2)) * unit, head), head)
        q_s[pl.ds(pl.multiple_of(i * tokens, tokens), tokens), :] = turned(acc_s[:, cols])

    e = head**-0.5 * LOG2E
    top_s[...] = jnp.full(top_s.shape, NEG, jnp.float32)
    mix_s[...] = jnp.zeros(mix_s.shape, jnp.float32)

    few = heads // 2

    def block(first, count, masked, begin):
        base = pl.multiple_of(first * tokens, tokens)
        at = [pl.ds(pl.multiple_of((begin + i) * tokens, tokens), tokens) for i in range(few)]
        keys = kv_s[pl.ds(base, count * tokens), :head]
        if masked:
            ok = lax.broadcasted_iota(jnp.int32, (tokens, tokens), 0) <= lax.broadcasted_iota(jnp.int32, (tokens, tokens), 1)
        values = jnp.concatenate([kv_s[pl.ds(base + j * part, part), head:] for j in range(2 * count)], axis=1)
        values = jnp.concatenate([values, jnp.ones((8, count * tokens), jnp.bfloat16)], axis=0)

        def score(i):
            s = _dot(keys, q_s[at[i], :], 1, 1)
            return jnp.where(ok, s, HIDDEN) if masked else s

        def soft(i, s):
            old = top_s[:, at[i]]
            top = jnp.maximum(old, s.max(axis=0, keepdims=True))
            top_s[:, at[i]] = top
            return jnp.exp2((s - top) * e).astype(jnp.bfloat16), jnp.exp2((old - top) * e)

        def mix(i, weight, keep):
            mix_s[:, at[i]] = mix_s[:, at[i]] * keep + _dot(values, weight, 1, 0)

        s0 = score(0)
        s1 = score(1)
        w0 = soft(0, s0)
        s2 = score(2)
        w1 = soft(1, s1)
        mix(0, *w0)
        s3 = score(3)
        w2 = soft(2, s2)
        mix(1, *w1)
        w3 = soft(3, s3)
        mix(2, *w2)
        mix(3, *w3)

    for which in (0, 1):
        if which == 1:
            arrive_x(W1, 5)
            arrive_x(W1, 6)
            shared(3)
            shared(4)
            arrive(KV, 0)
            arrive(WO, 0, False)
        lax.fori_loop(which * few, (which + 1) * few, turn, None)
        block(me, 1, True, which * few)
        if which == 0:
            own_to_mate(KV, False).wait_recv()

        @pl.when(core == 1)
        def _():
            block(me - 1, 1, False, which * few)

    def step(t, _):
        def one(j, _):
            way, which = j // 2, j % 2

            for slot in sorted({slot for slot, _, _ in RELAYS}):
                @pl.when((t == slot[0]) & (j == slot[1]))
                def _():
                    for kind, n in (entry[1:] for entry in RELAYS if entry[0] == slot):
                        if kind == X:
                            arrive_x(WO, n)
                        elif n < 0:
                            begin(WO, (1,))
                        elif kind == ON:
                            forward(WO, n)
                        else:
                            arrive(kind, n, kind == KV)

            @pl.when((t < 4) & (j == 0))
            def _():
                from_mate(KV, t)

            @pl.when((t == 4) & (j == 0))
            def _():
                from_mate(KV, 4)

            of = _chip((place + (8 - t) * (1 - way) + t * way) % 8)

            @pl.when((of < chip) & ((way == 0) | (t < 4)))
            def _():
                block(of * 2, 2, False, which * few)

        lax.fori_loop(0, 4, one, None)

    lax.fori_loop(1, 5, step, None)

    def finish(h, _):
        at = pl.ds(pl.multiple_of(h * tokens, tokens), tokens)
        total = mix_s[head : head + 1, at]
        a_s[:, pl.ds(pl.multiple_of(head_of(h) * head, head), head)] = (mix_s[:head, at] * (1 / total)).T.astype(jnp.bfloat16)

    arrive(WO, 6)
    lax.fori_loop(0, heads, finish, None)

    def output(chips, fresh=False, last=False):
        rows = [pl.ds(pl.multiple_of(c * 2 * depth, 2 * depth), 2 * depth) for c in chips]

        def tile(n, _):
            cols = pl.ds(pl.multiple_of(n * unit, unit), unit)
            total = x_s[:, cols].astype(jnp.float32) if fresh else acc_s[:, cols]
            total += functools.reduce(jnp.add, [_dot(a_s[:, r], wo_s[r, cols], 1, 0) for r in rows])
            if last:
                out_ref[:, cols] = total.astype(jnp.bfloat16)
            else:
                acc_s[:, cols] = total

        lax.fori_loop(0, dim // unit, tile, None)

    own_to_mate(WO, False).wait_recv()
    begun = sum(kind == X for _, kind, _ in RELAYS)
    t = 1
    for n in range(begun - 1, PIECES):
        if n >= begun:
            arrive_x(WO, n)
        while t < 4 and 2 * t - 1 <= n - (n >= begun):
            from_mate(WO, t)
            x_from_mate(WO, t)
            output([*([chip] if t == 1 else []), *(origin(way, t) for way in ways(t))], fresh=t == 1)
            t += 1
    from_mate(WO, 4)
    x_from_mate(WO, 4)
    output([origin(CW, 4)], last=True)

    for kind in (W1, KV, WO):
        own_to_mate(kind, True).wait_send()
        bulk(kind, 2 * PIECES, ring_cols(kind), ring_send.at[kind], d_recv.at[kind, 0]).wait_send()
        bulk(kind, 2 * PIECES, ring_cols(kind), d_send.at[kind], d_recv.at[kind, 0]).wait_send()
        if kind != KV:
            bulk(kind, 2 * x_pieces(kind), x_cols(kind, group), x_send.at[kind // 2], d_recv.at[kind, 0]).wait_send()
            bulk(kind, 2 * x_pieces(kind), x_cols(kind, 1 - group), dx_send.at[kind // 2], d_recv.at[kind, 0]).wait_send()


def attend(x, gain, wq, wk, wv, wo):
    half = wk.shape[1] // 2
    rate = THETA ** (-jnp.arange(half, dtype=jnp.float32) / half)
    (tokens, dim), depth, head = x.shape, wq.shape[0], wk.shape[1]
    heads = dim // head
    anywhere, vmem = pl.BlockSpec(memory_space=pl.ANY), pl.BlockSpec(memory_space=pltpu.VMEM)
    return pl.pallas_call(
        functools.partial(_kernel, shift={W1: 7 * dim // 16, WO: 7 * dim // 16}),
        out_shape=pltpu.VMEM((tokens, dim), jnp.bfloat16),
        in_specs=[anywhere, vmem, vmem, anywhere, anywhere, anywhere, anywhere],
        out_specs=vmem,
        scratch_shapes=[
            *[pltpu.VMEM((tokens, head // 2), jnp.float32)] * 2,
            pltpu.VMEM((tokens, dim), jnp.bfloat16),
            pltpu.VMEM((tokens, dim), jnp.bfloat16),
            pltpu.VMEM((16 * depth, dim + 2 * head), jnp.bfloat16),
            pltpu.VMEM((16 * depth, dim), jnp.bfloat16),
            pltpu.VMEM((16 * tokens, 2 * head), jnp.bfloat16),
            pltpu.VMEM((tokens, dim + 2 * head), jnp.float32),
            pltpu.VMEM((heads * tokens, head), jnp.bfloat16),
            pltpu.VMEM((1, heads * tokens), jnp.float32),
            pltpu.VMEM((head + 8, heads * tokens), jnp.float32),
            pltpu.SemaphoreType.DMA((6,)),
            *[pltpu.SemaphoreType.DMA(n) for n in ((3,), (3, 2, PIECES), (2,), (2, 2, PIECES), (3,), (3,), (3, 5), (2,), (2, 5))],
        ],
        compiler_params=pltpu.CompilerParams(collective_id=0, has_side_effects=True, vmem_limit_bytes=60 * 2**20),
    )(x, gain, rate[None], wq, wk, wv, wo)


def solution(mesh):
    tokens, whole = P(("dp", "sp"), None), P("sp", None)
    return jax.shard_map(
        attend,
        mesh=mesh,
        in_specs=(tokens, P(None), whole, whole, whole, whole),
        out_specs=tokens,
        check_vma=False,
    )
```
